32 devices in a mesh: patch: 16 (over z, y, core), chan: 2 (over x).
Axes of the slice: x: 2, y: 2, z: 4, core: 2. Of those that a mesh axis runs over, the one named last changes fastest.
Arguments:
- tokens: bfloat16 [1, 8192, 1280], P(None, 'patch'), may hold values from -12 to 12
- stale_k: bfloat16 [1, 8192, 1024], P(None, 'patch', 'chan'), may hold values from -64 to 64
- stale_v: bfloat16 [1, 8192, 1024], P(None, 'patch', 'chan'), may hold values from -6 to 6
- w_query: bfloat16 [1280, 1024], P(None, 'chan'), may hold values from -0.15625 to 0.15625
- w_key: bfloat16 [1280, 1024], P(None, 'chan'), may hold values from -0.4375 to 0.4375
- w_value: bfloat16 [1280, 1024], P(None, 'chan'), may hold values from -0.15625 to 0.15625
- w_out: bfloat16 [1024, 1280], P('chan'), may hold values from -0.1875 to 0.1875
- ff_value: bfloat16 [1280, 5120], P(None, 'chan'), may hold values from -0.15625 to 0.15625
- ff_gate: bfloat16 [1280, 5120], P(None, 'chan'), may hold values from -0.15625 to 0.15625
- ff_down: bfloat16 [5120, 1280], P('chan'), may hold values from -0.078125 to 0.078125
Outputs:
- layer_out: bfloat16 [1, 8192, 1280], P(None, 'patch', 'chan')
The draws below stay inside these ranges and needn't reach their ends.
All inputs are finite; a program needn't handle non-finite values.
Results may differ from the reference program's by a relative error of at most 0.0095.
Values may be sent and summed in bfloat16 or wider, within the bound.
No kernel may reach another device: no remote copies, remote signals or barrier semaphores. Data moves between devices by JAX's collectives and lax.ppermute only.
A program may use at most 128 MiB of HBM per device.

```python
import math
import jax
import jax.numpy as jnp
from jax import lax

D = 1280
HEADS = 16
HD = 64
FF = 5120
TOK_DEV = 512
BATCH = 1
TOKENS = 8192
N_PATCH = 16


def draw_tokens(key, part):
    key_base, key_cols = jax.random.split(jax.random.fold_in(key, 11), 2)
    shape = (BATCH, TOKENS, D)
    columns = jnp.exp(jax.random.uniform(key_cols, (D,), jnp.float32, math.log(0.3), math.log(3.0)))
    base = jax.random.normal(key_base, shape, jnp.float32) * columns
    return jnp.clip(base, -12.0, 12.0).astype(jnp.bfloat16)


def draw_stale_k(key, part):
    key_base = jax.random.fold_in(jax.random.fold_in(key, 23), 0)
    shape = (BATCH, TOKENS, HEADS * HD)
    base = jnp.clip(2.5 * jax.random.normal(key_base, shape, jnp.float32), -10.0, 10.0)
    return base.astype(jnp.bfloat16)


def block_scale(stream_key, shape, pieces, least, largest):
    level, own = 1.0, jax.random.fold_in(stream_key, 6)
    for axis_at, blocks in pieces:
        draws = jnp.exp(jax.random.uniform(jax.random.fold_in(own, axis_at), (blocks,), jnp.float32, least / len(pieces), largest / len(pieces)))
        level = level * jnp.repeat(draws, shape[axis_at] // blocks).reshape([-1 if axis == axis_at else 1 for axis in range(len(shape))])
    return level


def gaussian(rng, shape, scale, limit, cuts=(), held_as=jnp.bfloat16):
    values = jax.random.normal(rng, shape, jnp.float32) * scale
    if len(cuts) > 0:
        values = block_scale(rng, shape, cuts, -0.22, 0.18) * values
    return jnp.clip(values, min=-limit, max=limit).astype(held_as)


def setup_inputs(seed: int = 0) -> dict:
    key_list = jax.random.split(jax.random.key(seed), 11)
    tokens = draw_tokens(jax.random.fold_in(key_list[10], 71), 0)
    stale_k = draw_stale_k(jax.random.fold_in(key_list[10], 71), 0)
    stale_v = gaussian(key_list[2], (BATCH, TOKENS, HEADS * HD), 1.0, 6.0, ((1, 16), (2, 2)))
    w_query = gaussian(key_list[3], (D, HEADS * HD), D ** -0.5, 0.15625, ((1, 2),))
    w_key = gaussian(key_list[4], (D, HEADS * HD), (D // 6) ** -0.5, 0.4375, ((1, 2),))
    w_value = gaussian(key_list[5], (D, HEADS * HD), D ** -0.5, 0.15625, ((1, 2),))
    w_out = gaussian(key_list[6], (HEADS * HD, D), (HEADS * HD) ** -0.5, 0.1875, ((0, 2),))
    ff_value = gaussian(key_list[7], (D, FF), D ** -0.5, 0.15625, ((1, 2),))
    ff_gate = gaussian(key_list[8], (D, FF), D ** -0.5, 0.15625, ((1, 2),))
    ff_down = gaussian(key_list[9], (FF, D), FF ** -0.5, 0.078125, ((0, 2),))
    return {"tokens": tokens, "stale_k": stale_k, "stale_v": stale_v, "w_query": w_query, "w_key": w_key, "w_value": w_value, "w_out": w_out, "ff_value": ff_value, "ff_gate": ff_gate, "ff_down": ff_down}


def layer_norm(values):
    mean = lax.optimization_barrier(jnp.mean(values, axis=-1, keepdims=True))
    centered = values - mean
    var = lax.optimization_barrier(jnp.mean(centered * centered, axis=-1, keepdims=True))
    return centered * lax.rsqrt(var + 1e-05)

def to_wide(values):
    return lax.optimization_barrier(values).astype(jnp.float32)

def project(inputs, weight):
    return jnp.einsum('btd,de->bte', inputs.astype(jnp.float32), weight.astype(jnp.float32))

def reference(tokens, stale_k, stale_v, w_query, w_key, w_value, w_out, ff_value, ff_gate, ff_down):
    normed = layer_norm(tokens.astype(jnp.float32)).astype(jnp.bfloat16)
    queries = project(to_wide(normed), w_query).astype(jnp.bfloat16)
    key_fresh = project(to_wide(normed), w_key).astype(jnp.bfloat16)
    value_fresh = project(to_wide(normed), w_value).astype(jnp.bfloat16)
    shape_four = (BATCH, TOKENS, HEADS, HD)
    queries = queries.reshape(shape_four)
    key_fresh = key_fresh.reshape(shape_four)
    value_fresh = value_fresh.reshape(shape_four)
    stale_keys = stale_k.reshape(shape_four)
    stale_values = stale_v.reshape(shape_four)
    score_scale = 1.0 / HD ** 0.5

    def per_patch(patch_id):
        first_row = (patch_id * TOK_DEV).astype(jnp.int32)
        query_rows = lax.dynamic_slice_in_dim(queries, first_row, TOK_DEV, 1)
        fresh_keys = lax.dynamic_slice_in_dim(key_fresh, first_row, TOK_DEV, 1)
        fresh_values = lax.dynamic_slice_in_dim(value_fresh, first_row, TOK_DEV, 1)
        key_rows = lax.dynamic_update_slice_in_dim(stale_keys, fresh_keys, first_row, 1)
        value_rows = lax.dynamic_update_slice_in_dim(stale_values, fresh_values, first_row, 1)
        scores = jnp.einsum('bqhd,bkhd->bhqk', to_wide(query_rows), to_wide(key_rows)) * score_scale
        running_max = lax.optimization_barrier(jnp.max(scores, axis=-1, keepdims=True))
        weights = jnp.exp(scores - running_max)
        totals = lax.optimization_barrier(jnp.sum(weights, axis=-1))
        rounded = to_wide(weights.astype(jnp.bfloat16))
        accum = jnp.einsum('bhqk,bkhd->bhqd', rounded, to_wide(value_rows))
        result = accum / totals[..., None]
        return jnp.transpose(result, (0, 2, 1, 3)).reshape(BATCH, TOK_DEV, HEADS * HD)
    patches = lax.map(per_patch, jnp.arange(N_PATCH, dtype=jnp.int32))
    attended = jnp.transpose(patches, (1, 0, 2, 3)).reshape(BATCH, TOKENS, HEADS * HD).astype(jnp.bfloat16)
    resid = tokens.astype(jnp.float32) + project(to_wide(attended), w_out)
    normed_two = layer_norm(resid).astype(jnp.bfloat16)
    ff_val = project(to_wide(normed_two), ff_value)
    gate_out = project(to_wide(normed_two), ff_gate)
    gated = (ff_val * jax.nn.gelu(gate_out, approximate=False)).astype(jnp.bfloat16)
    layer_out = resid + project(to_wide(gated), ff_down)
    return layer_out.astype(jnp.bfloat16)
```

```python
import functools

import jax
import jax.numpy as jnp
from jax import lax
from jax.experimental import pallas as pl
from jax.experimental.pallas import tpu as pltpu
from jax.sharding import PartitionSpec as P

HD = 64
LANES = 128
NEG = -1e30
VMEM_BYTES = 60 * 2**20


def dot_nt(a, b):
    return lax.dot_general(a, b, (((1,), (1,)), ((), ())), preferred_element_type=jnp.float32)


def dot_nn(a, b):
    return jnp.dot(a, b, preferred_element_type=jnp.float32)


def swap(x):
    return jnp.concatenate([x[:, HD:], x[:, :HD]], axis=1)


def low_half(shape):
    return lax.broadcasted_iota(jnp.int32, shape, 1) < HD


def layer_norm(values):
    mean = jnp.mean(values, axis=-1, keepdims=True)
    centered = values - mean
    var = jnp.mean(centered * centered, axis=-1, keepdims=True)
    return centered * lax.rsqrt(var + 1e-05)


def whole(shape):
    return pl.BlockSpec(shape, lambda *_: (0,) * len(shape))


def params(**more):
    return pltpu.CompilerParams(vmem_limit_bytes=VMEM_BYTES, **more)


def cost(flops, moved, trans=0):
    return pl.CostEstimate(flops=int(flops), bytes_accessed=int(moved), transcendentals=int(trans))


def head_tile(ref, head):
    return ref[:, pl.ds(pl.multiple_of((head // 2) * LANES, LANES), LANES)]


def pack_kv(member, step, k_ref, v_ref, store):
    head = jnp.bitwise_xor(member, step)

    def put(odd):
        k_tile, v_tile = head_tile(k_ref, head), head_tile(v_ref, head)
        low = low_half(k_tile.shape)
        store(jnp.where(low, swap(k_tile), v_tile) if odd else jnp.where(low, k_tile, swap(v_tile)))

    pl.when(head % 2 == 0)(lambda: put(False))
    pl.when(head % 2 == 1)(lambda: put(True))


def pack_kernel(group, member_ref, k_ref, v_ref, *out_refs):
    for step in range(group):
        out = out_refs[step]

        def store(value, out=out):
            out[...] = value

        pack_kv(member_ref[0], step, k_ref, v_ref, store)


def pack_stale(member, stale_k, stale_v, group):
    rows, width = stale_k.shape
    packet = jax.ShapeDtypeStruct((rows, LANES), jnp.bfloat16)
    return pl.pallas_call(
        functools.partial(pack_kernel, group),
        in_specs=[
            pl.BlockSpec(memory_space=pltpu.SMEM),
            pl.BlockSpec(memory_space=pltpu.VMEM),
            pl.BlockSpec(memory_space=pltpu.VMEM),
        ],
        out_specs=[pl.BlockSpec(memory_space=pltpu.VMEM)] * group,
        out_shape=[packet] * group,
        compiler_params=params(),
        cost_estimate=cost(2e9, 4 * rows * width * 2),
        name="pack_stale",
    )(member, stale_k, stale_v)


def qkv_kernel(group, member_ref, x_ref, wq_hbm, wk_hbm, wv_hbm, *rest):
    out_refs, (wq, wk, wv, qs, ks, vs, sems) = rest[:group], rest[group:]
    copies = [
        pltpu.make_async_copy(src, dst, sems.at[at])
        for at, (src, dst) in enumerate(((wq_hbm, wq), (wk_hbm, wk), (wv_hbm, wv)))
    ]
    for copy in copies:
        copy.start()
    normed = layer_norm(x_ref[...].astype(jnp.float32)).astype(jnp.bfloat16)
    copies[0].wait()
    qs[...] = (dot_nn(normed, wq[...]).astype(jnp.bfloat16) * (1.0 / HD**0.5)).astype(jnp.bfloat16)
    copies[1].wait()
    ks[...] = dot_nn(normed, wk[...]).astype(jnp.bfloat16)
    copies[2].wait()
    vs[...] = dot_nn(normed, wv[...]).astype(jnp.bfloat16)
    rows = x_ref.shape[0]
    half = rows // 2
    member = member_ref[0]
    for step in range(group):
        out = out_refs[step]
        head = jnp.bitwise_xor(member, step)

        def put(odd, out=out, head=head):
            tile = head_tile(qs, head)
            low = low_half((half, LANES))
            first, second = tile[:half], tile[half:]
            if odd:
                out[:half, :] = jnp.where(low, swap(first), second)
            else:
                out[:half, :] = jnp.where(low, first, swap(second))

        pl.when(head % 2 == 0)(functools.partial(put, False))
        pl.when(head % 2 == 1)(functools.partial(put, True))

        def store(value, out=out):
            out[half:, :] = value

        pack_kv(member, step, ks, vs, store)


def project_qkv(member, tokens, w_query, w_key, w_value, group):
    rows, width = tokens.shape
    out_width = w_query.shape[1]
    packet = jax.ShapeDtypeStruct((rows // 2 + rows, LANES), jnp.bfloat16)
    return pl.pallas_call(
        functools.partial(qkv_kernel, group),
        in_specs=[
            pl.BlockSpec(memory_space=pltpu.SMEM),
            pl.BlockSpec(memory_space=pltpu.VMEM),
        ]
        + [pl.BlockSpec(memory_space=pltpu.HBM)] * 3,
        out_specs=[pl.BlockSpec(memory_space=pltpu.VMEM)] * group,
        out_shape=[packet] * group,
        scratch_shapes=[pltpu.VMEM((width, out_width), jnp.bfloat16)] * 3
        + [pltpu.VMEM((rows, out_width), jnp.bfloat16)] * 3
        + [pltpu.SemaphoreType.DMA((3,))],
        compiler_params=params(),
        cost_estimate=cost(6 * rows * width * out_width, 2 * 3 * width * out_width),
        name="project_qkv",
    )(member, tokens, w_query, w_key, w_value)


def attend_kernel(first, count, blocks, kv_rows, *refs):
    kv_hbm, refs = refs[:blocks], refs[blocks:]
    qf_hbm, refs = refs[:count], refs[count:]
    out_refs, (kvs, ones_v, qfs, kv_sems, qf_sems) = refs[:count], refs[count:]
    at = pl.program_id(0)
    half = out_refs[0].shape[0]
    low_kv = low_half((kv_rows, LANES))
    low_q = low_half((half, LANES))

    @pl.when(at == 0)
    def _():
        copies = [
            pltpu.make_async_copy(kv_hbm[b], kvs.at[b], kv_sems.at[b]) for b in range(blocks)
        ] + [pltpu.make_async_copy(qf_hbm[i], qfs.at[i], qf_sems.at[i]) for i in range(count)]
        for copy in copies:
            copy.start()
        for b in range(blocks):
            copies[b].wait()
            block = kvs[b]
            ones_v[b] = jnp.where(low_kv, jnp.ones_like(block), block)
        for i in range(count):
            copies[blocks + i].wait()

    own = first + at
    packed = qfs[at, :half, :]
    fresh = qfs[at, half:, :]
    fresh_v = jnp.where(low_kv, jnp.ones_like(fresh), fresh)
    zero = jnp.zeros_like(packed)
    picks = [b + (b >= own).astype(jnp.int32) for b in range(blocks - 1)]
    results = []
    for queries in (jnp.where(low_q, packed, zero), jnp.where(low_q, swap(packed), zero)):
        scores = [dot_nt(queries, kvs[pick]) for pick in picks] + [dot_nt(queries, fresh)]
        top = scores[0]
        for block in scores[1:]:
            top = jnp.maximum(top, block)
        top = jnp.max(top, axis=1, keepdims=True)
        accum = None
        for b, block in enumerate(scores):
            weights = jnp.exp(block - top).astype(jnp.bfloat16)
            part = dot_nn(weights, ones_v[picks[b]] if b < blocks - 1 else fresh_v)
            accum = part if accum is None else accum + part
        results.append(accum / swap(accum))
    value = jnp.where(low_q, swap(results[0]), results[1]).astype(jnp.bfloat16)
    for i in range(count):

        @pl.when(at == i)
        def _(i=i):
            out_refs[i][...] = value


def attend(first, queries, kv_blocks):
    count, blocks = len(queries), len(kv_blocks)
    kv_rows = kv_blocks[0].shape[0]
    packet_rows = queries[0].shape[0]
    half = packet_rows - kv_rows
    pairs = count * 2 * half * blocks * kv_rows
    return pl.pallas_call(
        functools.partial(attend_kernel, first, count, blocks, kv_rows),
        grid=(count,),
        in_specs=[pl.BlockSpec(memory_space=pltpu.HBM)] * (blocks + count),
        out_specs=[whole((half, LANES))] * count,
        out_shape=[jax.ShapeDtypeStruct((half, LANES), jnp.bfloat16)] * count,
        scratch_shapes=[
            pltpu.VMEM((blocks, kv_rows, LANES), jnp.bfloat16),
            pltpu.VMEM((blocks, kv_rows, LANES), jnp.bfloat16),
            pltpu.VMEM((count, packet_rows, LANES), jnp.bfloat16),
            pltpu.SemaphoreType.DMA((blocks,)),
            pltpu.SemaphoreType.DMA((count,)),
        ],
        compiler_params=params(dimension_semantics=("arbitrary",)),
        cost_estimate=cost(4 * pairs * LANES, 2 * blocks * kv_rows * LANES, pairs),
        name=f"attend_{first}",
    )(*kv_blocks, *queries)


def ffn_kernel(groups, chans, member_ref, tokens_ref, *refs):
    count = len(groups)
    packets, refs = refs[: chans * count], refs[chans * count :]
    w_out_refs, refs = refs[:chans], refs[chans:]
    val_ref, gate_ref, resid_ref, gated_ref, heads, normed_two = refs
    rows = tokens_ref.shape[0]
    half = rows // 2

    @pl.when(pl.program_id(0) == 0)
    def _():
        member = member_ref[0]
        low = low_half((half, LANES))
        for c in range(chans):
            for at, (start, size) in enumerate(groups):
                ref = packets[c * count + at]
                for pair in range(size // 2):
                    tile = jnp.bitwise_xor(member // 2, start // 2 + pair)
                    columns = pl.ds(pl.multiple_of(tile * LANES, LANES), LANES)

                    def put(odd, ref=ref, pair=pair, columns=columns, c=c):
                        one = ref[2 * pair * half : (2 * pair + 1) * half, :]
                        two = ref[(2 * pair + 1) * half : (2 * pair + 2) * half, :]
                        even_head, odd_head = (two, one) if odd else (one, two)
                        heads[c, :half, columns] = jnp.where(low, even_head, swap(odd_head))
                        heads[c, half:, columns] = jnp.where(low, swap(even_head), odd_head)

                    pl.when(member % 2 == 0)(functools.partial(put, False))
                    pl.when(member % 2 == 1)(functools.partial(put, True))
        resid = tokens_ref[...].astype(jnp.float32)
        for c in range(chans):
            resid = resid + dot_nn(heads[c], w_out_refs[c][...])
        resid_ref[...] = resid
        normed_two[...] = layer_norm(resid).astype(jnp.bfloat16)

    ff_val = dot_nn(normed_two[...], val_ref[...])
    gate = dot_nn(normed_two[...], gate_ref[...])
    gelu = 0.5 * gate * (1.0 + lax.erf(gate * (0.5**0.5)))
    gated_ref[...] = (ff_val * gelu).astype(jnp.bfloat16)


def out_and_ffn(member, tokens, packets, w_outs, ff_value, ff_gate, groups):
    rows, width = tokens.shape
    hidden = ff_value.shape[1]
    block = next(size for size in (512, 256, 128, hidden) if hidden % size == 0)
    chans = len(w_outs)
    heads_width = w_outs[0].shape[0]
    flat = [packet for chan in packets for packet in chan]
    return pl.pallas_call(
        functools.partial(ffn_kernel, groups, chans),
        grid=(hidden // block,),
        in_specs=[pl.BlockSpec(memory_space=pltpu.SMEM), whole(tokens.shape)]
        + [whole(packet.shape) for packet in flat]
        + [whole(w.shape) for w in w_outs]
        + [pl.BlockSpec((width, block), lambda i: (0, i))] * 2,
        out_specs=[whole((rows, width)), pl.BlockSpec((rows, block), lambda i: (0, i))],
        out_shape=[
            jax.ShapeDtypeStruct((rows, width), jnp.float32),
            jax.ShapeDtypeStruct((rows, hidden), jnp.bfloat16),
        ],
        scratch_shapes=[
            pltpu.VMEM((chans, rows, heads_width), jnp.bfloat16),
            pltpu.VMEM((rows, width), jnp.bfloat16),
        ],
        compiler_params=params(dimension_semantics=("arbitrary",)),
        cost_estimate=cost(4 * rows * width * hidden, 4 * width * hidden, rows * hidden),
        name="out_and_ffn",
    )(member, tokens, *flat, *w_outs, ff_value, ff_gate)


def down_kernel(target_ref, gated_ref, down_ref, out_ref, total):
    at = pl.program_id(0)
    part = dot_nn(gated_ref[...], down_ref[...])

    @pl.when(at == 0)
    def _():
        total[...] = part

    @pl.when(at > 0)
    def _():
        total[...] += part

    @pl.when(at == pl.num_programs(0) - 1)
    def _():
        out_ref[...] = total[...].astype(out_ref.dtype)


def down_project(target, gated, ff_down, share, dtype):
    rows, hidden = gated.shape
    if share % LANES != 0:
        ff_down = lax.dynamic_slice_in_dim(ff_down, target * share, share, 1)
        target = jnp.zeros_like(target)
    block = next(size for size in (1280, 640, 512, 256, 128, hidden) if hidden % size == 0)
    return pl.pallas_call(
        down_kernel,
        grid_spec=pltpu.PrefetchScalarGridSpec(
            num_scalar_prefetch=1,
            grid=(hidden // block,),
            in_specs=[
                pl.BlockSpec((rows, block), lambda k, target: (0, k)),
                pl.BlockSpec((block, share), lambda k, target: (k, target[0])),
            ],
            out_specs=pl.BlockSpec((rows, share), lambda k, target: (0, 0)),
            scratch_shapes=[pltpu.VMEM((rows, share), jnp.float32)],
        ),
        out_shape=jax.ShapeDtypeStruct((rows, share), dtype),
        compiler_params=params(dimension_semantics=("arbitrary",)),
        cost_estimate=cost(2 * rows * hidden * share, 2 * hidden * share),
        name="down_project",
    )(target.reshape(1), gated, ff_down)


def image_block(
    tokens, stale_k, stale_v, w_query, w_key, w_value, w_outs, ff_value, ff_gate, ff_down
):
    width = tokens.shape[1]
    head_count = w_query.shape[1] // HD
    patches = lax.axis_size("patch")
    chans = lax.axis_size("chan")
    group = 1
    while head_count % (2 * group) == 0 and patches % (2 * group) == 0:
        group *= 2
    assert group == head_count and group >= 2
    peers = patches // group
    patch_id = lax.axis_index("patch")
    chan_id = lax.axis_index("chan")
    member = (patch_id // peers).astype(jnp.int32).reshape(1)

    def trade(value, step):
        if step == 0:
            return value
        pairs = [(p, ((p // peers) ^ step) * peers + p % peers) for p in range(patches)]
        return lax.ppermute(value, "patch", pairs)

    def beside(value, step):
        pairs = [
            (p, p // peers * peers + (p % peers + step) % peers) for p in range(patches)
        ]
        return lax.ppermute(value, "patch", pairs)

    def over_chan(value, step):
        return lax.ppermute(value, "chan", [(c, (c + step) % chans) for c in range(chans)])

    stale_packets = pack_stale(member, stale_k, stale_v, group)
    kv_near = [trade(stale_packets[step], step) for step in range(group)]
    fresh_packets = project_qkv(member, tokens, w_query, w_key, w_value, group)
    queries = [trade(fresh_packets[step], step) for step in range(group)]
    kv_blocks = list(kv_near)
    for step in range(1, peers):
        kv_blocks += [beside(block, step) for block in kv_near]

    groups = [(0, 4), (4, 2), (6, 2)] if group == 8 else [(0, group)]
    packets = [[] for _ in range(chans)]
    for start, size in groups:
        heads = attend(start, queries[start : start + size], kv_blocks)
        mine = [trade(value, start + at) for at, value in enumerate(heads)]
        joined = jnp.concatenate(mine, axis=0)
        for step in range(chans):
            packets[step].append(joined if step == 0 else over_chan(joined, step))
    resid, gated = out_and_ffn(member, tokens, packets, w_outs, ff_value, ff_gate, groups)

    share = width // chans
    arrived = []
    for step in range(1, chans):
        target = ((chan_id + step) % chans).astype(jnp.int32)
        part = down_project(target, gated, ff_down, share, jnp.bfloat16)
        arrived.append(over_chan(part, step))
    total = down_project(chan_id.astype(jnp.int32), gated, ff_down, share, jnp.float32)
    total = total + lax.dynamic_slice_in_dim(resid, chan_id * share, share, 1)
    for part in arrived:
        total = total + part.astype(jnp.float32)
    return total.astype(jnp.bfloat16)


def per_device(
    tokens, stale_k, stale_v, w_query, w_key, w_value, w_out, ff_value, ff_gate, ff_down
):
    chans = lax.axis_size("chan")
    w_outs = [w_out] + [
        lax.ppermute(w_out, "chan", [(c, (c + step) % chans) for c in range(chans)])
        for step in range(1, chans)
    ]
    images = [
        image_block(
            tokens[at],
            stale_k[at],
            stale_v[at],
            w_query,
            w_key,
            w_value,
            w_outs,
            ff_value,
            ff_gate,
            ff_down,
        )
        for at in range(tokens.shape[0])
    ]
    return jnp.stack(images)


def solution(mesh):
    return jax.shard_map(
        per_device,
        mesh=mesh,
        in_specs=(
            P(None, "patch", None),
            P(None, "patch", "chan"),
            P(None, "patch", "chan"),
            P(None, "chan"),
            P(None, "chan"),
            P(None, "chan"),
            P("chan", None),
            P(None, "chan"),
            P(None, "chan"),
            P("chan", None),
        ),
        out_specs=P(None, "patch", "chan"),
        check_vma=False,
    )
```

```python
import functools

import jax
import jax.numpy as jnp
from jax import lax
from jax.experimental import pallas as pl
from jax.experimental.pallas import tpu as pltpu
from jax.sharding import PartitionSpec as P


HD = 64
LANES = 128


def dot_nt(a, b):
    return lax.dot_general(a, b, (((1,), (1,)), ((), ())), preferred_element_type=jnp.float32)


def dot_nn(a, b):
    return jnp.dot(a, b, preferred_element_type=jnp.float32)


def swap(x):
    return jnp.concatenate([x[:, HD:], x[:, :HD]], axis=1)


def low_half(shape):
    return lax.broadcasted_iota(jnp.int32, shape, 1) < HD


def layer_norm(values):
    mean = jnp.mean(values, axis=-1, keepdims=True)
    centered = values - mean
    var = jnp.mean(centered * centered, axis=-1, keepdims=True)
    return centered * lax.rsqrt(var + 1e-05)


def whole(shape):
    return pl.BlockSpec(shape, lambda *_: (0,) * len(shape))


def params(mib, **more):
    return pltpu.CompilerParams(vmem_limit_bytes=mib * 2**20, **more)


def cost(flops, moved, trans=0):
    return pl.CostEstimate(flops=int(flops), bytes_accessed=int(moved), transcendentals=int(trans))


def head_tile(ref, head):
    return ref[:, pl.ds(pl.multiple_of((head // 2) * LANES, LANES), LANES)]


def pack_kv(member, step, k_ref, v_ref, store):
    head = jnp.bitwise_xor(member, step)

    def put(odd):
        k_tile, v_tile = head_tile(k_ref, head), head_tile(v_ref, head)
        low = low_half(k_tile.shape)
        store(jnp.where(low, swap(k_tile), v_tile) if odd else jnp.where(low, k_tile, swap(v_tile)))

    pl.when(head % 2 == 0)(lambda: put(False))
    pl.when(head % 2 == 1)(lambda: put(True))


def pack_kernel(steps, member_ref, k_ref, v_ref, *out_refs):
    for step, out in zip(steps, out_refs):

        def store(value, out=out):
            out[...] = value

        pack_kv(member_ref[0], step, k_ref, v_ref, store)


def pack_stale(member, stale_k, stale_v, steps):
    rows, width = stale_k.shape
    packet = jax.ShapeDtypeStruct((rows, LANES), jnp.bfloat16)
    return pl.pallas_call(
        functools.partial(pack_kernel, steps),
        in_specs=[
            pl.BlockSpec(memory_space=pltpu.SMEM),
            pl.BlockSpec(memory_space=pltpu.VMEM),
            pl.BlockSpec(memory_space=pltpu.VMEM),
        ],
        out_specs=[pl.BlockSpec(memory_space=pltpu.VMEM)] * len(steps),
        out_shape=[packet] * len(steps),
        compiler_params=params(8),
        cost_estimate=cost(1e9, 4 * rows * width * 2),
        name="pack_stale",
    )(member, stale_k, stale_v)


def qkv_kernel(near, group, member_ref, x_ref, k_ref, v_ref, wq_hbm, wk_hbm, wv_hbm, *rest):
    out_refs, (wq, wk, wv, qs, ks, vs, sems) = rest[:group], rest[group:]
    copies = [
        pltpu.make_async_copy(src, dst, sems.at[at])
        for at, (src, dst) in enumerate(((wq_hbm, wq), (wk_hbm, wk), (wv_hbm, wv)))
    ]
    for copy in copies:
        copy.start()
    rows = x_ref.shape[0]
    half = rows // 2
    member = member_ref[0]
    for step in range(near):

        def store_stale(value, out=out_refs[step]):
            out[half + rows :, :] = value

        pack_kv(member, step, k_ref, v_ref, store_stale)
    normed = layer_norm(x_ref[...].astype(jnp.float32)).astype(jnp.bfloat16)
    copies[0].wait()
    qs[...] = (dot_nn(normed, wq[...]).astype(jnp.bfloat16) * (1.0 / HD**0.5)).astype(jnp.bfloat16)
    copies[1].wait()
    ks[...] = dot_nn(normed, wk[...]).astype(jnp.bfloat16)
    copies[2].wait()
    vs[...] = dot_nn(normed, wv[...]).astype(jnp.bfloat16)
    for step in range(group):
        out = out_refs[step]
        head = jnp.bitwise_xor(member, step)

        def put(odd, out=out, head=head):
            tile = head_tile(qs, head)
            low = low_half((half, LANES))
            first, second = tile[:half], tile[half:]
            if odd:
                out[:half, :] = jnp.where(low, swap(first), second)
            else:
                out[:half, :] = jnp.where(low, first, swap(second))

        pl.when(head % 2 == 0)(functools.partial(put, False))
        pl.when(head % 2 == 1)(functools.partial(put, True))

        def store(value, out=out):
            out[half : half + rows, :] = value

        pack_kv(member, step, ks, vs, store)


def project_qkv(member, tokens, stale_k, stale_v, w_query, w_key, w_value, near, group):
    rows, width = tokens.shape
    out_width = w_query.shape[1]
    return pl.pallas_call(
        functools.partial(qkv_kernel, near, group),
        in_specs=[pl.BlockSpec(memory_space=pltpu.SMEM)]
        + [pl.BlockSpec(memory_space=pltpu.VMEM)] * 3
        + [pl.BlockSpec(memory_space=pltpu.HBM)] * 3,
        out_specs=[pl.BlockSpec(memory_space=pltpu.VMEM)] * group,
        out_shape=[
            jax.ShapeDtypeStruct(
                (rows // 2 + rows * (2 if step < near else 1), LANES), jnp.bfloat16
            )
            for step in range(group)
        ],
        scratch_shapes=[pltpu.VMEM((width, out_width), jnp.bfloat16)] * 3
        + [pltpu.VMEM((rows, out_width), jnp.bfloat16)] * 3
        + [pltpu.SemaphoreType.DMA((3,))],
        compiler_params=params(60),
        cost_estimate=cost(6 * rows * width * out_width, 2 * 3 * width * out_width),
        name="project_qkv",
    )(member, tokens, stale_k, stale_v, w_query, w_key, w_value)


def attend_kernel(plan, *refs):
    count, blocks, queries, kv_rows = plan["count"], plan["blocks"], plan["queries"], plan["rows"]
    arrays, refs = refs[: plan["arrays"]], refs[plan["arrays"] :]
    state_in, refs = (refs[:2], refs[2:]) if plan["resume"] else (None, refs)
    outs = 2 if plan["partial"] else count
    out_refs, (kvs, ones_v, qfs) = refs[:outs], refs[outs:]
    at = pl.program_id(0)
    half = kv_rows // 2
    low_kv = low_half((kv_rows, LANES))
    low_q = low_half((half, LANES))

    @pl.when(at == 0)
    def _():
        for b, (ref, start) in enumerate(blocks):
            block = arrays[ref][start : start + kv_rows, :]
            kvs[b] = block
            ones_v[b] = jnp.where(low_kv, jnp.ones_like(block), block)
        for i, ref in enumerate(queries):
            qfs[i] = arrays[ref][: half + kv_rows, :]

    packed = qfs[at, :half, :]
    zero = jnp.zeros_like(packed)
    if plan["own"] is None:
        keys = [(kvs, ones_v, b) for b in range(len(blocks))]
    else:
        own = plan["own"] + at
        keys = [
            (kvs, ones_v, b + (b >= own).astype(jnp.int32)) for b in range(len(blocks) - 1)
        ]
    fresh, fresh_v = None, None
    if plan["own"] is not None:
        fresh = qfs[at, half:, :]
        fresh_v = jnp.where(low_kv, jnp.ones_like(fresh), fresh)
    results = []
    for side, query in enumerate(
        (jnp.where(low_q, packed, zero), jnp.where(low_q, swap(packed), zero))
    ):
        scores = [dot_nt(query, ref[pick]) for ref, _, pick in keys]
        if fresh is not None:
            scores.append(dot_nt(query, fresh))
        top = scores[0]
        for block in scores[1:]:
            top = jnp.maximum(top, block)
        top = jnp.max(top, axis=1, keepdims=True)
        accum = None
        for b, block in enumerate(scores):
            weights = jnp.exp(block - top).astype(jnp.bfloat16)
            part = dot_nn(weights, keys[b][1][keys[b][2]] if b < len(keys) else fresh_v)
            accum = part if accum is None else accum + part
        if plan["resume"]:
            accum_in, top_in = state_in[0][0, side], state_in[1][0, side]
            both = jnp.maximum(top_in, top)
            accum = accum_in * jnp.exp(top_in - both) + accum * jnp.exp(top - both)
        if plan["partial"]:
            out_refs[0][0, side] = accum
            out_refs[1][0, side] = jnp.broadcast_to(top, (half, LANES))
        else:
            results.append(accum / swap(accum))
    if not plan["partial"]:
        value = jnp.where(low_q, swap(results[0]), results[1]).astype(jnp.bfloat16)
        for i in range(count):

            @pl.when(at == i)
            def _(i=i):
                out_refs[i][...] = value


def attend(queries, kv_blocks, kv_rows, own, state=None, partial=False):
    arrays = []

    def place(value):
        for at, known in enumerate(arrays):
            if known is value:
                return at
        arrays.append(value)
        return len(arrays) - 1

    count = len(queries)
    half = kv_rows // 2
    plan = {
        "count": count,
        "queries": [place(query) for query in queries],
        "blocks": [(place(value), start) for value, start in kv_blocks],
        "rows": kv_rows,
        "own": own,
        "resume": state is not None,
        "partial": partial,
    }
    plan["arrays"] = len(arrays)
    blocks = len(kv_blocks)
    pairs = count * 2 * half * blocks * kv_rows
    carried = pl.BlockSpec((1, 2, half, LANES), lambda i: (i, 0, 0, 0))
    if partial:
        out_specs = [carried] * 2
        out_shape = [jax.ShapeDtypeStruct((count, 2, half, LANES), jnp.float32)] * 2
    else:
        out_specs = [whole((half, LANES))] * count
        out_shape = [jax.ShapeDtypeStruct((half, LANES), jnp.bfloat16)] * count
    return pl.pallas_call(
        functools.partial(attend_kernel, plan),
        grid=(count,),
        in_specs=[whole(value.shape) for value in arrays] + ([carried] * 2 if state else []),
        out_specs=out_specs,
        out_shape=out_shape,
        scratch_shapes=[
            pltpu.VMEM((blocks, kv_rows, LANES), jnp.bfloat16),
            pltpu.VMEM((blocks, kv_rows, LANES), jnp.bfloat16),
            pltpu.VMEM((count, half + kv_rows, LANES), jnp.bfloat16),
        ],
        compiler_params=params(4 + blocks * kv_rows // 186, dimension_semantics=("arbitrary",)),
        cost_estimate=cost(4 * pairs * LANES, 2 * blocks * kv_rows * LANES, pairs),
    )(*arrays, *(state or ()))


def ffn_kernel(spots, counts, aligned, scalars_ref, tokens_ref, *refs):
    arrays, chans = counts
    packets, refs = refs[:arrays], refs[arrays:]
    w_out_refs, refs = refs[:chans], refs[chans:]
    val_ref, gate_ref, down_hbm, resid_ref, gated_ref, part_ref, *refs = refs
    heads, normed_two, gated_all, down, sem = refs
    rows = tokens_ref.shape[0]
    half = rows // 2
    at, last = pl.program_id(0), pl.num_programs(0) - 1
    share = part_ref.shape[1]
    member, target, chan = scalars_ref[0], scalars_ref[1], scalars_ref[2]

    def columns(index, size):
        return pl.ds(pl.multiple_of(index * size, LANES), size)

    down_src = down_hbm.at[:, columns(target, share)] if aligned else down_hbm
    down_copy = pltpu.make_async_copy(down_src, down, sem)

    @pl.when(at == 0)
    def _():
        down_copy.start()
        low = low_half((half, LANES))
        for c in range(chans):
            for pair in range(len(spots[c]) // 2):
                place = columns(jnp.bitwise_xor(member // 2, pair), LANES)

                def put(odd, pair=pair, place=place, c=c):
                    one, two = (
                        packets[ref][start : start + half, :]
                        for ref, start in spots[c][2 * pair : 2 * pair + 2]
                    )
                    even_head, odd_head = (two, one) if odd else (one, two)
                    heads[c, :half, place] = jnp.where(low, even_head, swap(odd_head))
                    heads[c, half:, place] = jnp.where(low, swap(even_head), odd_head)

                pl.when(member % 2 == 0)(functools.partial(put, False))
                pl.when(member % 2 == 1)(functools.partial(put, True))
        resid = tokens_ref[...].astype(jnp.float32)
        for c in range(chans):
            resid = resid + dot_nn(heads[c], w_out_refs[c][...])
        if aligned:
            for c in range(chans):

                @pl.when(chan == c)
                def _(c=c):
                    resid_ref[...] = resid[:, c * share : (c + 1) * share]
        else:
            resid_ref[...] = resid
        normed_two[...] = layer_norm(resid).astype(jnp.bfloat16)

    ff_val = dot_nn(normed_two[...], val_ref[...])
    gate = dot_nn(normed_two[...], gate_ref[...])
    gelu = 0.5 * gate * (1.0 + lax.erf(gate * (0.5**0.5)))
    gated = (ff_val * gelu).astype(jnp.bfloat16)
    gated_ref[...] = gated
    block = gated.shape[1]
    gated_all[:, pl.ds(pl.multiple_of(at * block, LANES), block)] = gated

    @pl.when(at == last)
    def _():
        down_copy.wait()
        part_ref[...] = dot_nn(gated_all[...], down[...]).astype(part_ref.dtype)


def out_and_ffn(scalars, tokens, packets, w_outs, ff_value, ff_gate, ff_down, share):
    rows, width = tokens.shape
    hidden = ff_value.shape[1]
    block = next(size for size in (512, 256, 128) if hidden % size == 0)
    chans = len(w_outs)
    heads_width = w_outs[0].shape[0]
    arrays, spots = [], []
    for chan in packets:
        spots.append([])
        for value, start in chan:
            if not any(known is value for known in arrays):
                arrays.append(value)
            spots[-1].append((next(i for i, known in enumerate(arrays) if known is value), start))
    aligned = share % LANES == 0
    if not aligned:
        ff_down = lax.dynamic_slice_in_dim(ff_down, scalars[1] * share, share, 1)
    return pl.pallas_call(
        functools.partial(ffn_kernel, spots, (len(arrays), chans), aligned),
        grid=(hidden // block,),
        in_specs=[pl.BlockSpec(memory_space=pltpu.SMEM), whole(tokens.shape)]
        + [whole(value.shape) for value in arrays]
        + [whole(w.shape) for w in w_outs]
        + [pl.BlockSpec((width, block), lambda i: (0, i))] * 2
        + [pl.BlockSpec(memory_space=pltpu.HBM)],
        out_specs=[
            whole((rows, share if aligned else width)),
            pl.BlockSpec((rows, block), lambda i: (0, i)),
            whole((rows, share)),
        ],
        out_shape=[
            jax.ShapeDtypeStruct((rows, share if aligned else width), jnp.float32),
            jax.ShapeDtypeStruct((rows, hidden), jnp.bfloat16),
            jax.ShapeDtypeStruct((rows, share), jnp.bfloat16),
        ],
        scratch_shapes=[
            pltpu.VMEM((chans, rows, heads_width), jnp.bfloat16),
            pltpu.VMEM((rows, width), jnp.bfloat16),
            pltpu.VMEM((rows, hidden), jnp.bfloat16),
            pltpu.VMEM((hidden, share), jnp.bfloat16),
            pltpu.SemaphoreType.DMA,
        ],
        compiler_params=params(40, dimension_semantics=("arbitrary",)),
        cost_estimate=cost(4 * rows * width * hidden, 4 * width * hidden, rows * hidden),
        name="out_and_ffn",
    )(scalars, tokens, *arrays, *w_outs, ff_value, ff_gate, ff_down)


def down_kernel(target_ref, gated_ref, down_ref, out_ref, total):
    at = pl.program_id(0)
    part = dot_nn(gated_ref[...], down_ref[...])

    @pl.when(at == 0)
    def _():
        total[...] = part

    @pl.when(at > 0)
    def _():
        total[...] += part

    @pl.when(at == pl.num_programs(0) - 1)
    def _():
        out_ref[...] = total[...].astype(out_ref.dtype)


def down_project(target, gated, ff_down, share, dtype):
    rows, hidden = gated.shape
    if share % LANES != 0:
        ff_down = lax.dynamic_slice_in_dim(ff_down, target * share, share, 1)
        target = jnp.zeros_like(target)
    block = next(size for size in (1280, 640, 512, 256, 128, hidden) if hidden % size == 0)
    return pl.pallas_call(
        down_kernel,
        grid_spec=pltpu.PrefetchScalarGridSpec(
            num_scalar_prefetch=1,
            grid=(hidden // block,),
            in_specs=[
                pl.BlockSpec((rows, block), lambda k, target: (0, k)),
                pl.BlockSpec((block, share), lambda k, target: (k, target[0])),
            ],
            out_specs=pl.BlockSpec((rows, share), lambda k, target: (0, 0)),
            scratch_shapes=[pltpu.VMEM((rows, share), jnp.float32)],
        ),
        out_shape=jax.ShapeDtypeStruct((rows, share), dtype),
        compiler_params=params(20, dimension_semantics=("arbitrary",)),
        cost_estimate=cost(2 * rows * hidden * share, 2 * hidden * share),
        name="down_project",
    )(target.reshape(1), gated, ff_down)


def image_block(
    tokens, stale_k, stale_v, w_query, w_key, w_value, w_outs, ff_value, ff_gate, ff_down
):
    rows, width = tokens.shape
    head_count = w_query.shape[1] // HD
    patches = lax.axis_size("patch")
    chans = lax.axis_size("chan")
    group = 1
    while head_count % (2 * group) == 0 and patches % (2 * group) == 0:
        group *= 2
    assert group == head_count and group >= 2
    near = group // 2
    peers = patches // group
    patch_id = lax.axis_index("patch")
    chan_id = lax.axis_index("chan").astype(jnp.int32)
    member = (patch_id // peers).astype(jnp.int32).reshape(1)

    def partner(p, step):
        return ((p // peers) ^ step) * peers + p % peers

    def trade(value, step):
        if step == 0:
            return value
        return lax.ppermute(value, "patch", [(p, partner(p, step)) for p in range(patches)])

    def beside(value, step):
        pairs = [
            (p, p // peers * peers + (p % peers + step) % peers) for p in range(patches)
        ]
        return lax.ppermute(value, "patch", pairs)

    def over_chan(value, step):
        return lax.ppermute(value, "chan", [(c, (c + step) % chans) for c in range(chans)])

    def trade_over_chan(value, step, chan_step):
        if chan_step == 0:
            return trade(value, step)
        pairs = [
            (p * chans + c, partner(p, step) * chans + (c + chan_step) % chans)
            for p in range(patches)
            for c in range(chans)
        ]
        return lax.ppermute(value, ("patch", "chan"), pairs)

    made = project_qkv(
        member, tokens, stale_k, stale_v, w_query, w_key, w_value, near, group
    )
    nears = [trade(made[step], step) for step in range(near)]
    stale_far = pack_stale(member, stale_k, stale_v, tuple(range(near, group)))
    kv_far = [trade(stale_far[step - near], step) for step in range(near, group)]
    q_far = [trade(made[step], step) for step in range(near, group)]
    near_side = [[beside(value, step) for value in nears] for step in range(1, peers)]
    far_side = [[beside(value, step) for value in kv_far] for step in range(1, peers)]
    stale_at = rows // 2 + rows
    near_own = [(value, stale_at) for value in nears]
    near_rest = [(value, stale_at) for side in near_side for value in side]
    far_own = [(value, 0) for value in kv_far]
    far_rest = [(value, 0) for side in far_side for value in side]

    packets = [[] for _ in range(chans)]
    state = attend(nears, near_own + near_rest, rows, 0, partial=True)
    heads = attend(nears, far_own + far_rest, rows, None, state=state)
    if group > 2:
        mine = [trade(value, at) for at, value in enumerate(heads)]
        joined = jnp.concatenate(mine, axis=0)
        for step in range(chans):
            value = joined if step == 0 else over_chan(joined, step)
            packets[step] += [(value, at * (rows // 2)) for at in range(near)]
    else:
        for step in range(chans):
            for at, value in enumerate(heads):
                packets[step].append((trade_over_chan(value, at, step), 0))
    parts = 2 if group >= 8 else 1
    size = (group - near) // parts
    everything = far_own + near_own + far_rest + near_rest
    for part in range(parts):
        start = part * size
        asked = q_far[start : start + size]
        asked, heads = lax.optimization_barrier((asked, heads))
        heads = attend(asked, everything, rows, start)
        steps = range(near + start, near + start + size)
        if part < parts - 1:
            mine = [trade(value, at) for at, value in zip(steps, heads)]
            joined = jnp.concatenate(mine, axis=0)
            for step in range(chans):
                value = joined if step == 0 else over_chan(joined, step)
                packets[step] += [(value, at * (rows // 2)) for at in range(size)]
        else:
            for step in range(chans):
                for at, value in zip(steps, heads):
                    sent = trade_over_chan(value, at, step)
                    packets[step].append((sent, 0))

    share = width // chans
    target = (chan_id + 1) % chans
    scalars = jnp.stack([member[0], target, chan_id])
    resid, gated, part = out_and_ffn(
        scalars, tokens, packets, w_outs, ff_value, ff_gate, ff_down, share
    )
    arrived = [over_chan(part, 1)] if chans > 1 else []
    for step in range(2, chans):
        part = down_project((chan_id + step) % chans, gated, ff_down, share, jnp.bfloat16)
        arrived.append(over_chan(part, step))
    total = down_project(chan_id, gated, ff_down, share, jnp.float32)
    if resid.shape[1] != share:
        resid = lax.dynamic_slice_in_dim(resid, chan_id * share, share, 1)
    total = total + resid
    for part in arrived:
        total = total + part.astype(jnp.float32)
    return total.astype(jnp.bfloat16)


def per_device(
    tokens, stale_k, stale_v, w_query, w_key, w_value, w_out, ff_value, ff_gate, ff_down
):
    chans = lax.axis_size("chan")
    w_outs = [w_out]
    for step in range(1, chans):
        pairs = [(c, (c + step) % chans) for c in range(chans)]
        w_outs.append(lax.ppermute(w_out, "chan", pairs))
    images = [
        image_block(
            tokens[at],
            stale_k[at],
            stale_v[at],
            w_query,
            w_key,
            w_value,
            w_outs,
            ff_value,
            ff_gate,
            ff_down,
        )
        for at in range(tokens.shape[0])
    ]
    return jnp.stack(images)


def solution(mesh):
    return jax.shard_map(
        per_device,
        mesh=mesh,
        in_specs=(
            P(None, "patch", None),
            P(None, "patch", "chan"),
            P(None, "patch", "chan"),
            P(None, "chan"),
            P(None, "chan"),
            P(None, "chan"),
            P("chan", None),
            P(None, "chan"),
            P(None, "chan"),
            P("chan", None),
        ),
        out_specs=P(None, "patch", "chan"),
        check_vma=False,
    )
```

```python
import functools

import jax
import jax.numpy as jnp
from jax import lax
from jax.experimental import pallas as pl
from jax.experimental.pallas import tpu as pltpu
from jax.sharding import PartitionSpec as P


HD = 64
LANES = 128


def dot_nt(a, b):
    return lax.dot_general(a, b, (((1,), (1,)), ((), ())), preferred_element_type=jnp.float32)


def dot_nn(a, b):
    return jnp.dot(a, b, preferred_element_type=jnp.float32)


def swap(x):
    return jnp.concatenate([x[:, HD:], x[:, :HD]], axis=1)


def low_half(shape):
    return lax.broadcasted_iota(jnp.int32, shape, 1) < HD


def layer_norm(values):
    mean = jnp.mean(values, axis=-1, keepdims=True)
    centered = values - mean
    var = jnp.mean(centered * centered, axis=-1, keepdims=True)
    return centered * lax.rsqrt(var + 1e-05)


def whole(shape):
    return pl.BlockSpec(shape, lambda *_: (0,) * len(shape))


def params(mib, **more):
    return pltpu.CompilerParams(vmem_limit_bytes=mib * 2**20, **more)


def cost(flops, moved, trans=0):
    return pl.CostEstimate(flops=int(flops), bytes_accessed=int(moved), transcendentals=int(trans))


STAT_ROWS = 16


def write_result(out_ref, start, parts, with_stats):
    rows = parts[0][0].shape[0]
    low = low_half((rows, LANES))
    sides = [accum / swap(accum) for accum, _ in parts]
    out_ref[start : start + rows, :] = jnp.where(low, swap(sides[0]), sides[1]).astype(
        jnp.bfloat16
    )
    if not with_stats:
        return
    lane = lax.broadcasted_iota(jnp.int32, (rows, LANES), 1)
    table = jnp.zeros((rows, LANES), jnp.float32)
    for side, (accum, top) in enumerate(parts):
        rest = jnp.where(low, top + jnp.log(jnp.where(low, accum, 1.0)), 0.0)
        for part in range(3):
            piece = rest.astype(jnp.bfloat16).astype(jnp.float32)
            rest = rest - piece
            table = jnp.where(lane == 3 * side + part, piece, table)
    pick_shape = (STAT_ROWS, LANES)
    pick = lax.broadcasted_iota(jnp.int32, pick_shape, 0) == lax.broadcasted_iota(
        jnp.int32, pick_shape, 1
    )
    stats = dot_nt(
        jnp.where(pick, 1.0, 0.0).astype(jnp.bfloat16), table.astype(jnp.bfloat16)
    ).astype(jnp.bfloat16)
    for at in range(rows // LANES):
        first = start + rows + at * STAT_ROWS
        out_ref[first : first + STAT_ROWS, :] = stats[:, at * LANES : (at + 1) * LANES]


def result_rows(rows):
    return rows + rows // LANES * STAT_ROWS


def read_stats(ref, start, rows):
    stats = jnp.concatenate(
        [
            ref[start + rows + at * STAT_ROWS : start + rows + (at + 1) * STAT_ROWS, :]
            for at in range(rows // LANES)
        ],
        axis=1,
    )
    row = lax.broadcasted_iota(jnp.int32, (STAT_ROWS, LANES), 0)
    low = low_half((STAT_ROWS, LANES))
    spread = jnp.where((row < 3) & low | (row >= 3) & (row < 6) & ~low, 1.0, 0.0)
    return lax.dot_general(
        stats,
        spread.astype(jnp.bfloat16),
        (((0,), (0,)), ((), ())),
        preferred_element_type=jnp.float32,
    )


def merge_results(ref, start, local_ref, local_start, rows):
    one = ref[start : start + rows, :].astype(jnp.float32)
    two = local_ref[local_start : local_start + rows, :].astype(jnp.float32)
    gap = read_stats(local_ref, local_start, rows) - read_stats(ref, start, rows)
    share = 1.0 / (1.0 + jnp.exp(gap))
    return (two + (one - two) * share).astype(jnp.bfloat16)


def local_kernel(count, *refs):
    q_refs, fresh_refs, out_ref = refs[:count], refs[count : 2 * count], refs[2 * count]
    for at in range(count):
        packed, fresh = q_refs[at][...], fresh_refs[at][...]
        low = low_half(packed.shape)
        fresh_v = jnp.where(low_half(fresh.shape), jnp.ones_like(fresh), fresh)
        zero = jnp.zeros_like(packed)
        parts = []
        for query in (jnp.where(low, packed, zero), jnp.where(low, swap(packed), zero)):
            scores = dot_nt(query, fresh)
            top = jnp.max(scores, axis=1, keepdims=True)
            parts.append((dot_nn(jnp.exp(scores - top).astype(jnp.bfloat16), fresh_v), top))
        write_result(out_ref, at * result_rows(packed.shape[0]), parts, True)


def attend_local(queries, fresh):
    count, rows = len(queries), queries[0].shape[0]
    return pl.pallas_call(
        functools.partial(local_kernel, count),
        in_specs=[pl.BlockSpec(memory_space=pltpu.VMEM)] * (2 * count),
        out_specs=pl.BlockSpec(memory_space=pltpu.VMEM),
        out_shape=jax.ShapeDtypeStruct((count * result_rows(rows), LANES), jnp.bfloat16),
        compiler_params=params(16),
        cost_estimate=cost(16 * count * rows * rows * LANES, 8 * count * rows * LANES),
        name="attend_local",
    )(*queries, *fresh)


def head_tile(ref, head):
    return ref[:, pl.ds(pl.multiple_of((head // 2) * LANES, LANES), LANES)]


def pack_kv(member, step, k_ref, v_ref, store):
    head = jnp.bitwise_xor(member, step)

    def put(odd):
        k_tile, v_tile = head_tile(k_ref, head), head_tile(v_ref, head)
        low = low_half(k_tile.shape)
        store(jnp.where(low, swap(k_tile), v_tile) if odd else jnp.where(low, k_tile, swap(v_tile)))

    pl.when(head % 2 == 0)(lambda: put(False))
    pl.when(head % 2 == 1)(lambda: put(True))


def pack_kernel(steps, member_ref, k_ref, v_ref, *out_refs):
    for step, out in zip(steps, out_refs):

        def store(value, out=out):
            out[...] = value

        pack_kv(member_ref[0], step, k_ref, v_ref, store)


def pack_stale(member, stale_k, stale_v, steps):
    rows, width = stale_k.shape
    packet = jax.ShapeDtypeStruct((rows, LANES), jnp.bfloat16)
    return pl.pallas_call(
        functools.partial(pack_kernel, steps),
        in_specs=[
            pl.BlockSpec(memory_space=pltpu.SMEM),
            pl.BlockSpec(memory_space=pltpu.VMEM),
            pl.BlockSpec(memory_space=pltpu.VMEM),
        ],
        out_specs=[pl.BlockSpec(memory_space=pltpu.VMEM)] * len(steps),
        out_shape=[packet] * len(steps),
        compiler_params=params(8),
        cost_estimate=cost(1e9, 4 * rows * width * 2),
        name="pack_stale",
    )(member, stale_k, stale_v)


def qkv_kernel(near, group, member_ref, x_ref, k_ref, v_ref, wq_hbm, wk_hbm, wv_hbm, *rest):
    out_refs, rest = rest[:group], rest[group:]
    fresh_refs, (wq, wk, wv, qs, ks, vs, sems) = rest[: group - near], rest[group - near :]
    copies = [
        pltpu.make_async_copy(src, dst, sems.at[at])
        for at, (src, dst) in enumerate(((wq_hbm, wq), (wk_hbm, wk), (wv_hbm, wv)))
    ]
    for copy in copies:
        copy.start()
    rows = x_ref.shape[0]
    half = rows // 2
    member = member_ref[0]
    for step in range(near):

        def store_stale(value, out=out_refs[step]):
            out[half + rows :, :] = value

        pack_kv(member, step, k_ref, v_ref, store_stale)
    normed = layer_norm(x_ref[...].astype(jnp.float32)).astype(jnp.bfloat16)
    copies[0].wait()
    qs[...] = (dot_nn(normed, wq[...]).astype(jnp.bfloat16) * (1.0 / HD**0.5)).astype(jnp.bfloat16)
    copies[1].wait()
    ks[...] = dot_nn(normed, wk[...]).astype(jnp.bfloat16)
    copies[2].wait()
    vs[...] = dot_nn(normed, wv[...]).astype(jnp.bfloat16)
    for step in range(group):
        out = out_refs[step]
        head = jnp.bitwise_xor(member, step)

        def put(odd, out=out, head=head):
            tile = head_tile(qs, head)
            low = low_half((half, LANES))
            first, second = tile[:half], tile[half:]
            if odd:
                out[:half, :] = jnp.where(low, swap(first), second)
            else:
                out[:half, :] = jnp.where(low, first, swap(second))

        pl.when(head % 2 == 0)(functools.partial(put, False))
        pl.when(head % 2 == 1)(functools.partial(put, True))

        def store(value, out=out, step=step):
            if step < near:
                out[half : half + rows, :] = value
            else:
                fresh_refs[step - near][...] = value

        pack_kv(member, step, ks, vs, store)


def project_qkv(member, tokens, stale_k, stale_v, w_query, w_key, w_value, near, group):
    rows, width = tokens.shape
    out_width = w_query.shape[1]
    return pl.pallas_call(
        functools.partial(qkv_kernel, near, group),
        in_specs=[pl.BlockSpec(memory_space=pltpu.SMEM)]
        + [pl.BlockSpec(memory_space=pltpu.VMEM)] * 3
        + [pl.BlockSpec(memory_space=pltpu.HBM)] * 3,
        out_specs=[pl.BlockSpec(memory_space=pltpu.VMEM)] * (2 * group - near),
        out_shape=[
            jax.ShapeDtypeStruct((size, LANES), jnp.bfloat16)
            for size in [rows // 2 + 2 * rows] * near
            + [rows // 2] * (group - near)
            + [rows] * (group - near)
        ],
        scratch_shapes=[pltpu.VMEM((width, out_width), jnp.bfloat16)] * 3
        + [pltpu.VMEM((rows, out_width), jnp.bfloat16)] * 3
        + [pltpu.SemaphoreType.DMA((3,))],
        compiler_params=params(60),
        cost_estimate=cost(6 * rows * width * out_width, 2 * 3 * width * out_width),
        name="project_qkv",
    )(member, tokens, stale_k, stale_v, w_query, w_key, w_value)


def attend_kernel(plan, *refs):
    count, blocks, queries, kv_rows = plan["count"], plan["blocks"], plan["queries"], plan["rows"]
    arrays, refs = refs[: plan["arrays"]], refs[plan["arrays"] :]
    state_in, refs = (refs[:2], refs[2:]) if plan["resume"] else (None, refs)
    outs = 2 if plan["partial"] else count
    out_refs, (kvs, ones_v, qfs, result) = refs[:outs], refs[outs:]
    at = pl.program_id(0)
    half = kv_rows // 2
    low_kv = low_half((kv_rows, LANES))
    low_q = low_half((half, LANES))
    q_rows = qfs.shape[1]

    @pl.when(at == 0)
    def _():
        for b, (ref, start) in enumerate(blocks):
            block = arrays[ref][start : start + kv_rows, :]
            kvs[b] = block
            ones_v[b] = jnp.where(low_kv, jnp.ones_like(block), block)
        for i, ref in enumerate(queries):
            qfs[i] = arrays[ref][:q_rows, :]

    packed = qfs[at, :half, :]
    zero = jnp.zeros_like(packed)
    if plan["own"] is None:
        keys = [(kvs, ones_v, b) for b in range(len(blocks))]
    else:
        own = plan["own"] + at
        keys = [
            (kvs, ones_v, b + (b >= own).astype(jnp.int32)) for b in range(len(blocks) - 1)
        ]
    fresh, fresh_v = None, None
    if plan["fresh"]:
        fresh = qfs[at, half:, :]
        fresh_v = jnp.where(low_kv, jnp.ones_like(fresh), fresh)
    results = []
    for side, query in enumerate(
        (jnp.where(low_q, packed, zero), jnp.where(low_q, swap(packed), zero))
    ):
        scores = [dot_nt(query, ref[pick]) for ref, _, pick in keys]
        if fresh is not None:
            scores.append(dot_nt(query, fresh))
        top = scores[0]
        for block in scores[1:]:
            top = jnp.maximum(top, block)
        top = jnp.max(top, axis=1, keepdims=True)
        accum = None
        for b, block in enumerate(scores):
            weights = jnp.exp(block - top).astype(jnp.bfloat16)
            part = dot_nn(weights, keys[b][1][keys[b][2]] if b < len(keys) else fresh_v)
            accum = part if accum is None else accum + part
        if plan["resume"]:
            accum_in, top_in = state_in[0][0, side], state_in[1][0, side]
            both = jnp.maximum(top_in, top)
            accum = accum_in * jnp.exp(top_in - both) + accum * jnp.exp(top - both)
        if plan["partial"]:
            out_refs[0][0, side] = accum
            out_refs[1][0, side] = jnp.broadcast_to(top, (half, LANES))
        else:
            results.append((accum, top))
    if not plan["partial"]:
        write_result(result, 0, results, plan["stats"])
        for i in range(count):

            @pl.when(at == i)
            def _(i=i):
                out_refs[i][...] = result[: out_refs[i].shape[0], :]


def attend(queries, kv_blocks, kv_rows, own, fresh, state=None, partial=False, stats=False):
    arrays = []

    def place(value):
        for at, known in enumerate(arrays):
            if known is value:
                return at
        arrays.append(value)
        return len(arrays) - 1

    count = len(queries)
    half = kv_rows // 2
    plan = {
        "count": count,
        "queries": [place(query) for query in queries],
        "blocks": [(place(value), start) for value, start in kv_blocks],
        "rows": kv_rows,
        "own": own,
        "resume": state is not None,
        "partial": partial,
        "fresh": fresh,
        "stats": stats,
    }
    plan["arrays"] = len(arrays)
    blocks = len(kv_blocks)
    pairs = count * 2 * half * blocks * kv_rows
    carried = pl.BlockSpec((1, 2, half, LANES), lambda i: (i, 0, 0, 0))
    if partial:
        out_specs = [carried] * 2
        out_shape = [jax.ShapeDtypeStruct((count, 2, half, LANES), jnp.float32)] * 2
    else:
        packet = (result_rows(half) if stats else half, LANES)
        out_specs = [whole(packet)] * count
        out_shape = [jax.ShapeDtypeStruct(packet, jnp.bfloat16)] * count
    return pl.pallas_call(
        functools.partial(attend_kernel, plan),
        grid=(count,),
        in_specs=[whole(value.shape) for value in arrays] + ([carried] * 2 if state else []),
        out_specs=out_specs,
        out_shape=out_shape,
        scratch_shapes=[
            pltpu.VMEM((blocks, kv_rows, LANES), jnp.bfloat16),
            pltpu.VMEM((blocks, kv_rows, LANES), jnp.bfloat16),
            pltpu.VMEM((count, half + kv_rows if fresh else half, LANES), jnp.bfloat16),
            pltpu.VMEM((result_rows(half), LANES), jnp.bfloat16),
        ],
        compiler_params=params(4 + blocks * kv_rows // 186, dimension_semantics=("arbitrary",)),
        cost_estimate=cost(4 * pairs * LANES, 2 * blocks * kv_rows * LANES, pairs),
    )(*arrays, *(state or ()))


def ffn_kernel(spots, counts, aligned, scalars_ref, tokens_ref, *refs):
    arrays, chans = counts
    packets, refs = refs[:arrays], refs[arrays:]
    w_out_refs, refs = refs[:chans], refs[chans:]
    val_ref, gate_ref, down_hbm, resid_ref, gated_ref, part_ref, *refs = refs
    heads, normed_two, gated_all, down, sem = refs
    rows = tokens_ref.shape[0]
    half = rows // 2
    at, last = pl.program_id(0), pl.num_programs(0) - 1
    share = part_ref.shape[1]
    member, target, chan = scalars_ref[0], scalars_ref[1], scalars_ref[2]

    def columns(index, size):
        return pl.ds(pl.multiple_of(index * size, LANES), size)

    down_src = down_hbm.at[:, columns(target, share)] if aligned else down_hbm
    down_copy = pltpu.make_async_copy(down_src, down, sem)

    @pl.when(at == 0)
    def _():
        down_copy.start()
        low = low_half((half, LANES))
        for c in range(chans):
            for pair in range(len(spots[c]) // 2):
                place = columns(jnp.bitwise_xor(member // 2, pair), LANES)

                def put(odd, pair=pair, place=place, c=c):
                    one, two = (
                        packets[ref][start : start + half, :]
                        if local is None
                        else merge_results(packets[ref], start, packets[local], local_start, half)
                        for ref, start, local, local_start in spots[c][2 * pair : 2 * pair + 2]
                    )
                    even_head, odd_head = (two, one) if odd else (one, two)
                    heads[c, :half, place] = jnp.where(low, even_head, swap(odd_head))
                    heads[c, half:, place] = jnp.where(low, swap(even_head), odd_head)

                pl.when(member % 2 == 0)(functools.partial(put, False))
                pl.when(member % 2 == 1)(functools.partial(put, True))
        resid = tokens_ref[...].astype(jnp.float32)
        for c in range(chans):
            resid = resid + dot_nn(heads[c], w_out_refs[c][...])
        if aligned:
            for c in range(chans):

                @pl.when(chan == c)
                def _(c=c):
                    resid_ref[...] = resid[:, c * share : (c + 1) * share]
        else:
            resid_ref[...] = resid
        normed_two[...] = layer_norm(resid).astype(jnp.bfloat16)

    ff_val = dot_nn(normed_two[...], val_ref[...])
    gate = dot_nn(normed_two[...], gate_ref[...])
    gelu = 0.5 * gate * (1.0 + lax.erf(gate * (0.5**0.5)))
    gated = (ff_val * gelu).astype(jnp.bfloat16)
    gated_ref[...] = gated
    block = gated.shape[1]
    gated_all[:, pl.ds(pl.multiple_of(at * block, LANES), block)] = gated

    @pl.when(at == last)
    def _():
        down_copy.wait()
        part_ref[...] = dot_nn(gated_all[...], down[...]).astype(part_ref.dtype)


def out_and_ffn(scalars, tokens, packets, w_outs, ff_value, ff_gate, ff_down, share):
    rows, width = tokens.shape
    hidden = ff_value.shape[1]
    block = next(size for size in (512, 256, 128) if hidden % size == 0)
    chans = len(w_outs)
    heads_width = w_outs[0].shape[0]
    arrays, spots = [], []

    def place(value):
        if value is None:
            return None
        for at, known in enumerate(arrays):
            if known is value:
                return at
        arrays.append(value)
        return len(arrays) - 1

    for chan in packets:
        spots.append([])
        for value, start, local, local_start in chan:
            spots[-1].append((place(value), start, place(local), local_start))
    aligned = share % LANES == 0
    if not aligned:
        ff_down = lax.dynamic_slice_in_dim(ff_down, scalars[1] * share, share, 1)
    return pl.pallas_call(
        functools.partial(ffn_kernel, spots, (len(arrays), chans), aligned),
        grid=(hidden // block,),
        in_specs=[pl.BlockSpec(memory_space=pltpu.SMEM), whole(tokens.shape)]
        + [whole(value.shape) for value in arrays]
        + [whole(w.shape) for w in w_outs]
        + [pl.BlockSpec((width, block), lambda i: (0, i))] * 2
        + [pl.BlockSpec(memory_space=pltpu.HBM)],
        out_specs=[
            whole((rows, share if aligned else width)),
            pl.BlockSpec((rows, block), lambda i: (0, i)),
            whole((rows, share)),
        ],
        out_shape=[
            jax.ShapeDtypeStruct((rows, share if aligned else width), jnp.float32),
            jax.ShapeDtypeStruct((rows, hidden), jnp.bfloat16),
            jax.ShapeDtypeStruct((rows, share), jnp.bfloat16),
        ],
        scratch_shapes=[
            pltpu.VMEM((chans, rows, heads_width), jnp.bfloat16),
            pltpu.VMEM((rows, width), jnp.bfloat16),
            pltpu.VMEM((rows, hidden), jnp.bfloat16),
            pltpu.VMEM((hidden, share), jnp.bfloat16),
            pltpu.SemaphoreType.DMA,
        ],
        compiler_params=params(40, dimension_semantics=("arbitrary",)),
        cost_estimate=cost(4 * rows * width * hidden, 4 * width * hidden, rows * hidden),
        name="out_and_ffn",
    )(scalars, tokens, *arrays, *w_outs, ff_value, ff_gate, ff_down)


def down_kernel(target_ref, gated_ref, down_ref, out_ref, total):
    at = pl.program_id(0)
    part = dot_nn(gated_ref[...], down_ref[...])

    @pl.when(at == 0)
    def _():
        total[...] = part

    @pl.when(at > 0)
    def _():
        total[...] += part

    @pl.when(at == pl.num_programs(0) - 1)
    def _():
        out_ref[...] = total[...].astype(out_ref.dtype)


def down_project(target, gated, ff_down, share, dtype):
    rows, hidden = gated.shape
    if share % LANES != 0:
        ff_down = lax.dynamic_slice_in_dim(ff_down, target * share, share, 1)
        target = jnp.zeros_like(target)
    block = next(size for size in (1280, 640, 512, 256, 128, hidden) if hidden % size == 0)
    return pl.pallas_call(
        down_kernel,
        grid_spec=pltpu.PrefetchScalarGridSpec(
            num_scalar_prefetch=1,
            grid=(hidden // block,),
            in_specs=[
                pl.BlockSpec((rows, block), lambda k, target: (0, k)),
                pl.BlockSpec((block, share), lambda k, target: (k, target[0])),
            ],
            out_specs=pl.BlockSpec((rows, share), lambda k, target: (0, 0)),
            scratch_shapes=[pltpu.VMEM((rows, share), jnp.float32)],
        ),
        out_shape=jax.ShapeDtypeStruct((rows, share), dtype),
        compiler_params=params(20, dimension_semantics=("arbitrary",)),
        cost_estimate=cost(2 * rows * hidden * share, 2 * hidden * share),
        name="down_project",
    )(target.reshape(1), gated, ff_down)


def image_block(
    tokens, stale_k, stale_v, w_query, w_key, w_value, w_outs, ff_value, ff_gate, ff_down
):
    rows, width = tokens.shape
    head_count = w_query.shape[1] // HD
    patches = lax.axis_size("patch")
    chans = lax.axis_size("chan")
    group = 1
    while head_count % (2 * group) == 0 and patches % (2 * group) == 0:
        group *= 2
    assert group == head_count and group >= 2
    near = group // 2
    peers = patches // group
    patch_id = lax.axis_index("patch")
    chan_id = lax.axis_index("chan").astype(jnp.int32)
    member = (patch_id // peers).astype(jnp.int32).reshape(1)

    def partner(p, step):
        return ((p // peers) ^ step) * peers + p % peers

    def trade(value, step):
        if step == 0:
            return value
        return lax.ppermute(value, "patch", [(p, partner(p, step)) for p in range(patches)])

    def beside(value, step):
        pairs = [
            (p, p // peers * peers + (p % peers + step) % peers) for p in range(patches)
        ]
        return lax.ppermute(value, "patch", pairs)

    def over_chan(value, step):
        return lax.ppermute(value, "chan", [(c, (c + step) % chans) for c in range(chans)])

    def trade_over_chan(value, step, chan_step):
        if chan_step == 0:
            return trade(value, step)
        pairs = [
            (p * chans + c, partner(p, step) * chans + (c + chan_step) % chans)
            for p in range(patches)
            for c in range(chans)
        ]
        return lax.ppermute(value, ("patch", "chan"), pairs)

    made = project_qkv(
        member, tokens, stale_k, stale_v, w_query, w_key, w_value, near, group
    )
    nears = [trade(made[step], step) for step in range(near)]
    stale_far = pack_stale(member, stale_k, stale_v, tuple(range(near, group)))
    kv_far = [trade(stale_far[step - near], step) for step in range(near, group)]
    q_far = [trade(made[step], step) for step in range(near, group)]
    local = attend_local(made[near:group], made[group:])
    locals_ = [local if step == 0 else over_chan(local, step) for step in range(chans)]
    result_size = result_rows(rows // 2)
    near_side = [[beside(value, step) for value in nears] for step in range(1, peers)]
    far_side = [[beside(value, step) for value in kv_far] for step in range(1, peers)]
    stale_at = rows // 2 + rows
    near_own = [(value, stale_at) for value in nears]
    near_rest = [(value, stale_at) for side in near_side for value in side]
    far_own = [(value, 0) for value in kv_far]
    far_rest = [(value, 0) for side in far_side for value in side]

    packets = [[] for _ in range(chans)]
    state = attend(nears, near_own + near_rest, rows, 0, True, partial=True)
    heads = attend(nears, far_own + far_rest, rows, None, False, state=state)
    if group > 2:
        mine = [trade(value, at) for at, value in enumerate(heads)]
        joined = jnp.concatenate(mine, axis=0)
        for step in range(chans):
            value = joined if step == 0 else over_chan(joined, step)
            packets[step] += [(value, at * (rows // 2), None, 0) for at in range(near)]
    else:
        for step in range(chans):
            for at, value in enumerate(heads):
                sent = trade_over_chan(value, at, step)
                packets[step].append((sent, 0, None, 0))
    parts = 2 if group >= 8 else 1
    size = (group - near) // parts
    everything = far_own + near_own + far_rest + near_rest
    for part in range(parts):
        start = part * size
        asked = q_far[start : start + size]
        asked, heads = lax.optimization_barrier((asked, heads))
        heads = attend(asked, everything, rows, start, False, stats=True)
        steps = range(near + start, near + start + size)
        if part < parts - 1:
            mine = [trade(value, at) for at, value in zip(steps, heads)]
            joined = jnp.concatenate(mine, axis=0)
            for step in range(chans):
                value = joined if step == 0 else over_chan(joined, step)
                packets[step] += [
                    (value, at * result_size, locals_[step], (start + at) * result_size)
                    for at in range(size)
                ]
        else:
            for step in range(chans):
                for at, value in zip(steps, heads):
                    sent = trade_over_chan(value, at, step)
                    packets[step].append((sent, 0, locals_[step], (at - near) * result_size))

    share = width // chans
    target = (chan_id + 1) % chans
    scalars = jnp.stack([member[0], target, chan_id])
    resid, gated, part = out_and_ffn(
        scalars, tokens, packets, w_outs, ff_value, ff_gate, ff_down, share
    )
    arrived = [over_chan(part, 1)] if chans > 1 else []
    for step in range(2, chans):
        part = down_project((chan_id + step) % chans, gated, ff_down, share, jnp.bfloat16)
        arrived.append(over_chan(part, step))
    total = down_project(chan_id, gated, ff_down, share, jnp.float32)
    if resid.shape[1] != share:
        resid = lax.dynamic_slice_in_dim(resid, chan_id * share, share, 1)
    total = total + resid
    for part in arrived:
        total = total + part.astype(jnp.float32)
    return total.astype(jnp.bfloat16)


def per_device(
    tokens, stale_k, stale_v, w_query, w_key, w_value, w_out, ff_value, ff_gate, ff_down
):
    chans = lax.axis_size("chan")
    w_outs = [w_out]
    for step in range(1, chans):
        pairs = [(c, (c + step) % chans) for c in range(chans)]
        w_outs.append(lax.ppermute(w_out, "chan", pairs))
    images = [
        image_block(
            tokens[at],
            stale_k[at],
            stale_v[at],
            w_query,
            w_key,
            w_value,
            w_outs,
            ff_value,
            ff_gate,
            ff_down,
        )
        for at in range(tokens.shape[0])
    ]
    return jnp.stack(images)


def solution(mesh):
    return jax.shard_map(
        per_device,
        mesh=mesh,
        in_specs=(
            P(None, "patch", None),
            P(None, "patch", "chan"),
            P(None, "patch", "chan"),
            P(None, "chan"),
            P(None, "chan"),
            P(None, "chan"),
            P("chan", None),
            P(None, "chan"),
            P(None, "chan"),
            P("chan", None),
        ),
        out_specs=P(None, "patch", "chan"),
        check_vma=False,
    )
```

```python
import functools

import jax
import jax.numpy as jnp
from jax import lax
from jax.experimental import pallas as pl
from jax.experimental.pallas import tpu as pltpu
from jax.sharding import PartitionSpec as P


HD = 64
LANES = 128


def dot_nt(a, b):
    return lax.dot_general(a, b, (((1,), (1,)), ((), ())), preferred_element_type=jnp.float32)


def dot_nn(a, b):
    return jnp.dot(a, b, preferred_element_type=jnp.float32)


def swap(x):
    return jnp.concatenate([x[:, HD:], x[:, :HD]], axis=1)


def low_half(shape):
    return lax.broadcasted_iota(jnp.int32, shape, 1) < HD


def layer_norm(values):
    mean = jnp.mean(values, axis=-1, keepdims=True)
    centered = values - mean
    var = jnp.mean(centered * centered, axis=-1, keepdims=True)
    return centered * lax.rsqrt(var + 1e-05)


def whole(shape):
    return pl.BlockSpec(shape, lambda *_: (0,) * len(shape))


def params(mib, **more):
    return pltpu.CompilerParams(vmem_limit_bytes=mib * 2**20, **more)


def cost(flops, moved, trans=0):
    return pl.CostEstimate(flops=int(flops), bytes_accessed=int(moved), transcendentals=int(trans))


STAT_ROWS = 16


def write_result(out_ref, start, parts, with_stats):
    rows = parts[0][0].shape[0]
    low = low_half((rows, LANES))
    sides = [accum / swap(accum) for accum, _ in parts]
    out_ref[start : start + rows, :] = jnp.where(low, swap(sides[0]), sides[1]).astype(
        jnp.bfloat16
    )
    if not with_stats:
        return
    lane = lax.broadcasted_iota(jnp.int32, (rows, LANES), 1)
    table = jnp.zeros((rows, LANES), jnp.float32)
    for side, (accum, top) in enumerate(parts):
        rest = jnp.where(low, top + jnp.log(jnp.where(low, accum, 1.0)), 0.0)
        for part in range(3):
            piece = rest.astype(jnp.bfloat16).astype(jnp.float32)
            rest = rest - piece
            table = jnp.where(lane == 3 * side + part, piece, table)
    pick_shape = (STAT_ROWS, LANES)
    pick = lax.broadcasted_iota(jnp.int32, pick_shape, 0) == lax.broadcasted_iota(
        jnp.int32, pick_shape, 1
    )
    stats = dot_nt(
        jnp.where(pick, 1.0, 0.0).astype(jnp.bfloat16), table.astype(jnp.bfloat16)
    ).astype(jnp.bfloat16)
    for at in range(rows // LANES):
        first = start + rows + at * STAT_ROWS
        out_ref[first : first + STAT_ROWS, :] = stats[:, at * LANES : (at + 1) * LANES]


def result_rows(rows):
    return rows + rows // LANES * STAT_ROWS


def read_stats(ref, start, rows):
    stats = jnp.concatenate(
        [
            ref[start + rows + at * STAT_ROWS : start + rows + (at + 1) * STAT_ROWS, :]
            for at in range(rows // LANES)
        ],
        axis=1,
    )
    row = lax.broadcasted_iota(jnp.int32, (STAT_ROWS, LANES), 0)
    low = low_half((STAT_ROWS, LANES))
    spread = jnp.where((row < 3) & low | (row >= 3) & (row < 6) & ~low, 1.0, 0.0)
    return lax.dot_general(
        stats,
        spread.astype(jnp.bfloat16),
        (((0,), (0,)), ((), ())),
        preferred_element_type=jnp.float32,
    )


def merge_results(ref, start, local_ref, local_start, rows):
    one = ref[start : start + rows, :].astype(jnp.float32)
    two = local_ref[local_start : local_start + rows, :].astype(jnp.float32)
    gap = read_stats(local_ref, local_start, rows) - read_stats(ref, start, rows)
    share = 1.0 / (1.0 + jnp.exp(gap))
    return (two + (one - two) * share).astype(jnp.bfloat16)


def local_kernel(count, *refs):
    q_refs, fresh_refs = refs[:count], refs[count : 2 * count]
    out_ref, packed_ref, fresh_ref = refs[2 * count :]
    for at in range(count):

        @pl.when(pl.program_id(0) == at)
        def _(at=at):
            packed_ref[...] = q_refs[at][...]
            fresh_ref[...] = fresh_refs[at][...]

    packed, fresh = packed_ref[...], fresh_ref[...]
    low = low_half(packed.shape)
    fresh_v = jnp.where(low_half(fresh.shape), jnp.ones_like(fresh), fresh)
    zero = jnp.zeros_like(packed)
    parts = []
    for query in (jnp.where(low, packed, zero), jnp.where(low, swap(packed), zero)):
        scores = dot_nt(query, fresh)
        top = jnp.max(scores, axis=1, keepdims=True)
        parts.append((dot_nn(jnp.exp(scores - top).astype(jnp.bfloat16), fresh_v), top))
    write_result(out_ref, 0, parts, True)


def attend_local(queries, fresh):
    count, rows = len(queries), queries[0].shape[0]
    size = result_rows(rows)
    return pl.pallas_call(
        functools.partial(local_kernel, count),
        grid=(count,),
        in_specs=[whole(value.shape) for value in (*queries, *fresh)],
        out_specs=pl.BlockSpec((size, LANES), lambda i: (i, 0)),
        out_shape=jax.ShapeDtypeStruct((count * size, LANES), jnp.bfloat16),
        scratch_shapes=[
            pltpu.VMEM(queries[0].shape, jnp.bfloat16),
            pltpu.VMEM(fresh[0].shape, jnp.bfloat16),
        ],
        compiler_params=params(16, dimension_semantics=("arbitrary",)),
        cost_estimate=cost(16 * count * rows * rows * LANES, 8 * count * rows * LANES),
        name="attend_local",
    )(*queries, *fresh)


def head_tile(ref, head):
    return ref[:, pl.ds(pl.multiple_of((head // 2) * LANES, LANES), LANES)]


def pack_kv(member, step, k_ref, v_ref, store):
    head = jnp.bitwise_xor(member, step)

    def put(odd):
        k_tile, v_tile = head_tile(k_ref, head), head_tile(v_ref, head)
        low = low_half(k_tile.shape)
        store(jnp.where(low, swap(k_tile), v_tile) if odd else jnp.where(low, k_tile, swap(v_tile)))

    pl.when(head % 2 == 0)(lambda: put(False))
    pl.when(head % 2 == 1)(lambda: put(True))


def pack_kernel(steps, member_ref, k_ref, v_ref, *out_refs):
    for step, out in zip(steps, out_refs):

        def store(value, out=out):
            out[...] = value

        pack_kv(member_ref[0], step, k_ref, v_ref, store)


def pack_stale(member, stale_k, stale_v, steps):
    rows, width = stale_k.shape
    packet = jax.ShapeDtypeStruct((rows, LANES), jnp.bfloat16)
    return pl.pallas_call(
        functools.partial(pack_kernel, steps),
        in_specs=[
            pl.BlockSpec(memory_space=pltpu.SMEM),
            pl.BlockSpec(memory_space=pltpu.VMEM),
            pl.BlockSpec(memory_space=pltpu.VMEM),
        ],
        out_specs=[pl.BlockSpec(memory_space=pltpu.VMEM)] * len(steps),
        out_shape=[packet] * len(steps),
        compiler_params=params(8),
        cost_estimate=cost(1e9, 4 * rows * width * 2),
        name="pack_stale",
    )(member, stale_k, stale_v)


def qkv_kernel(near, group, member_ref, x_ref, k_ref, v_ref, wq_hbm, wk_hbm, wv_hbm, *rest):
    out_refs, rest = rest[:group], rest[group:]
    fresh_refs, (wq, wk, wv, qs, ks, vs, sems) = rest[: group - near], rest[group - near :]
    copies = [
        pltpu.make_async_copy(src, dst, sems.at[at])
        for at, (src, dst) in enumerate(((wq_hbm, wq), (wk_hbm, wk), (wv_hbm, wv)))
    ]
    for copy in copies:
        copy.start()
    rows = x_ref.shape[0]
    half = rows // 2
    member = member_ref[0]
    for step in range(near):

        def store_stale(value, out=out_refs[step]):
            out[half + rows :, :] = value

        pack_kv(member, step, k_ref, v_ref, store_stale)
    normed = layer_norm(x_ref[...].astype(jnp.float32)).astype(jnp.bfloat16)
    copies[0].wait()
    qs[...] = (dot_nn(normed, wq[...]).astype(jnp.bfloat16) * (1.0 / HD**0.5)).astype(jnp.bfloat16)
    copies[1].wait()
    ks[...] = dot_nn(normed, wk[...]).astype(jnp.bfloat16)
    copies[2].wait()
    vs[...] = dot_nn(normed, wv[...]).astype(jnp.bfloat16)
    for step in range(group):
        out = out_refs[step]
        head = jnp.bitwise_xor(member, step)

        def put(odd, out=out, head=head):
            tile = head_tile(qs, head)
            low = low_half((half, LANES))
            first, second = tile[:half], tile[half:]
            if odd:
                out[:half, :] = jnp.where(low, swap(first), second)
            else:
                out[:half, :] = jnp.where(low, first, swap(second))

        pl.when(head % 2 == 0)(functools.partial(put, False))
        pl.when(head % 2 == 1)(functools.partial(put, True))

        def store(value, out=out, step=step):
            if step < near:
                out[half : half + rows, :] = value
            else:
                fresh_refs[step - near][...] = value

        pack_kv(member, step, ks, vs, store)


def project_qkv(member, tokens, stale_k, stale_v, w_query, w_key, w_value, near, group):
    rows, width = tokens.shape
    out_width = w_query.shape[1]
    return pl.pallas_call(
        functools.partial(qkv_kernel, near, group),
        in_specs=[pl.BlockSpec(memory_space=pltpu.SMEM)]
        + [pl.BlockSpec(memory_space=pltpu.VMEM)] * 3
        + [pl.BlockSpec(memory_space=pltpu.HBM)] * 3,
        out_specs=[pl.BlockSpec(memory_space=pltpu.VMEM)] * (2 * group - near),
        out_shape=[
            jax.ShapeDtypeStruct((size, LANES), jnp.bfloat16)
            for size in [rows // 2 + 2 * rows] * near
            + [rows // 2] * (group - near)
            + [rows] * (group - near)
        ],
        scratch_shapes=[pltpu.VMEM((width, out_width), jnp.bfloat16)] * 3
        + [pltpu.VMEM((rows, out_width), jnp.bfloat16)] * 3
        + [pltpu.SemaphoreType.DMA((3,))],
        compiler_params=params(60),
        cost_estimate=cost(6 * rows * width * out_width, 2 * 3 * width * out_width),
        name="project_qkv",
    )(member, tokens, stale_k, stale_v, w_query, w_key, w_value)


def attend_kernel(plan, *refs):
    count, blocks, queries, kv_rows = plan["count"], plan["blocks"], plan["queries"], plan["rows"]
    arrays, refs = refs[: plan["arrays"]], refs[plan["arrays"] :]
    state_in, refs = (refs[:1], refs[1:]) if plan["resume"] else (None, refs)
    outs = 1 if plan["partial"] else count
    out_refs, (kvs, ones_v, qfs, result) = refs[:outs], refs[outs:]
    at = pl.program_id(0)
    half = kv_rows // 2
    low_kv = low_half((kv_rows, LANES))
    low_q = low_half((half, LANES))
    q_rows = qfs.shape[1]

    @pl.when(at == 0)
    def _():
        for b, (ref, start) in enumerate(blocks):
            block = arrays[ref][start : start + kv_rows, :]
            kvs[b] = block
            ones_v[b] = jnp.where(low_kv, jnp.ones_like(block), block)
        for i, ref in enumerate(queries):
            qfs[i] = arrays[ref][:q_rows, :]

    packed = qfs[at, :half, :]
    zero = jnp.zeros_like(packed)
    if plan["own"] is None:
        keys = [(kvs, ones_v, b) for b in range(len(blocks))]
    else:
        own = plan["own"] + at
        keys = [
            (kvs, ones_v, b + (b >= own).astype(jnp.int32)) for b in range(len(blocks) - 1)
        ]
    fresh, fresh_v = None, None
    if plan["fresh"]:
        fresh = qfs[at, half:, :]
        fresh_v = jnp.where(low_kv, jnp.ones_like(fresh), fresh)
    results = []
    for side, query in enumerate(
        (jnp.where(low_q, packed, zero), jnp.where(low_q, swap(packed), zero))
    ):
        scores = [dot_nt(query, ref[pick]) for ref, _, pick in keys]
        if fresh is not None:
            scores.append(dot_nt(query, fresh))
        top = scores[0]
        for block in scores[1:]:
            top = jnp.maximum(top, block)
        top = jnp.max(top, axis=1, keepdims=True)
        accum = None
        for b, block in enumerate(scores):
            weights = jnp.exp(block - top).astype(jnp.bfloat16)
            part = dot_nn(weights, keys[b][1][keys[b][2]] if b < len(keys) else fresh_v)
            accum = part if accum is None else accum + part
        if plan["resume"]:
            carried = state_in[0][0, side]
            top_in = carried[:, :1]
            accum_in = jnp.where(low_q, carried[:, HD - 1 : HD], carried)
            both = jnp.maximum(top_in, top)
            accum = accum_in * jnp.exp(top_in - both) + accum * jnp.exp(top - both)
        if plan["partial"]:
            lane = lax.broadcasted_iota(jnp.int32, (half, LANES), 1)
            out_refs[0][0, side] = jnp.where(lane < HD // 2, top, accum)
        else:
            results.append((accum, top))
    if not plan["partial"]:
        write_result(result, 0, results, plan["stats"])
        for i in range(count):

            @pl.when(at == i)
            def _(i=i):
                out_refs[i][...] = result[: out_refs[i].shape[0], :]


def attend(queries, kv_blocks, kv_rows, own, fresh, state=None, partial=False, stats=False):
    arrays = []

    def place(value):
        for at, known in enumerate(arrays):
            if known is value:
                return at
        arrays.append(value)
        return len(arrays) - 1

    count = len(queries)
    half = kv_rows // 2
    plan = {
        "count": count,
        "queries": [place(query) for query in queries],
        "blocks": [(place(value), start) for value, start in kv_blocks],
        "rows": kv_rows,
        "own": own,
        "resume": state is not None,
        "partial": partial,
        "fresh": fresh,
        "stats": stats,
    }
    plan["arrays"] = len(arrays)
    blocks = len(kv_blocks)
    pairs = count * 2 * half * blocks * kv_rows
    carried = pl.BlockSpec((1, 2, half, LANES), lambda i: (i, 0, 0, 0))
    if partial:
        out_specs = [carried]
        out_shape = [jax.ShapeDtypeStruct((count, 2, half, LANES), jnp.float32)]
    else:
        packet = (result_rows(half) if stats else half, LANES)
        out_specs = [whole(packet)] * count
        out_shape = [jax.ShapeDtypeStruct(packet, jnp.bfloat16)] * count
    return pl.pallas_call(
        functools.partial(attend_kernel, plan),
        grid=(count,),
        in_specs=[whole(value.shape) for value in arrays] + ([carried] if state else []),
        out_specs=out_specs,
        out_shape=out_shape,
        scratch_shapes=[
            pltpu.VMEM((blocks, kv_rows, LANES), jnp.bfloat16),
            pltpu.VMEM((blocks, kv_rows, LANES), jnp.bfloat16),
            pltpu.VMEM((count, half + kv_rows if fresh else half, LANES), jnp.bfloat16),
            pltpu.VMEM((result_rows(half), LANES), jnp.bfloat16),
        ],
        compiler_params=params(4 + blocks * kv_rows // 186, dimension_semantics=("arbitrary",)),
        cost_estimate=cost(4 * pairs * LANES, 2 * blocks * kv_rows * LANES, pairs),
    )(*arrays, *(state or ()))


def ffn_kernel(spots, counts, aligned, scalars_ref, tokens_ref, *refs):
    arrays, chans = counts
    packets, refs = refs[:arrays], refs[arrays:]
    w_out_refs, refs = refs[:chans], refs[chans:]
    val_ref, gate_ref, down_hbm, resid_ref, gated_ref, part_ref, *refs = refs
    heads, normed_two, gated_all, down, sem = refs
    rows = tokens_ref.shape[0]
    half = rows // 2
    at, last = pl.program_id(0), pl.num_programs(0) - 1
    share = part_ref.shape[1]
    member, target, chan = scalars_ref[0], scalars_ref[1], scalars_ref[2]

    def columns(index, size):
        return pl.ds(pl.multiple_of(index * size, LANES), size)

    down_src = down_hbm.at[:, columns(target, share)] if aligned else down_hbm
    down_copy = pltpu.make_async_copy(down_src, down, sem)

    @pl.when(at == 0)
    def _():
        down_copy.start()
        low = low_half((half, LANES))
        for c in range(chans):
            for pair in range(len(spots[c]) // 2):
                place = columns(jnp.bitwise_xor(member // 2, pair), LANES)

                def put(odd, pair=pair, place=place, c=c):
                    one, two = (
                        packets[ref][start : start + half, :]
                        if local is None
                        else merge_results(packets[ref], start, packets[local], local_start, half)
                        for ref, start, local, local_start in spots[c][2 * pair : 2 * pair + 2]
                    )
                    even_head, odd_head = (two, one) if odd else (one, two)
                    heads[c, :half, place] = jnp.where(low, even_head, swap(odd_head))
                    heads[c, half:, place] = jnp.where(low, swap(even_head), odd_head)

                pl.when(member % 2 == 0)(functools.partial(put, False))
                pl.when(member % 2 == 1)(functools.partial(put, True))
        resid = tokens_ref[...].astype(jnp.float32)
        for c in range(chans):
            resid = resid + dot_nn(heads[c], w_out_refs[c][...])
        if aligned:
            for c in range(chans):

                @pl.when(chan == c)
                def _(c=c):
                    resid_ref[...] = resid[:, c * share : (c + 1) * share]
        else:
            resid_ref[...] = resid
        normed_two[...] = layer_norm(resid).astype(jnp.bfloat16)

    block = gated_ref.shape[1]
    piece = 256 if block % 256 == 0 else block
    for start in range(0, block, piece):
        ff_val = dot_nn(normed_two[...], val_ref[:, start : start + piece])
        gate = dot_nn(normed_two[...], gate_ref[:, start : start + piece])
        gelu = 0.5 * gate * (1.0 + lax.erf(gate * (0.5**0.5)))
        gated = (ff_val * gelu).astype(jnp.bfloat16)
        gated_ref[:, start : start + piece] = gated
        gated_all[:, pl.ds(pl.multiple_of(at * block + start, LANES), piece)] = gated

    @pl.when(at == last)
    def _():
        down_copy.wait()
        part_ref[...] = dot_nn(gated_all[...], down[...]).astype(part_ref.dtype)


def out_and_ffn(scalars, tokens, packets, w_outs, ff_value, ff_gate, ff_down, share):
    rows, width = tokens.shape
    hidden = ff_value.shape[1]
    block = next(size for size in (512, 256, 128) if hidden % size == 0)
    chans = len(w_outs)
    heads_width = w_outs[0].shape[0]
    arrays, spots = [], []

    def place(value):
        if value is None:
            return None
        for at, known in enumerate(arrays):
            if known is value:
                return at
        arrays.append(value)
        return len(arrays) - 1

    for chan in packets:
        spots.append([])
        for value, start, local, local_start in chan:
            spots[-1].append((place(value), start, place(local), local_start))
    aligned = share % LANES == 0
    if not aligned:
        ff_down = lax.dynamic_slice_in_dim(ff_down, scalars[1] * share, share, 1)
    return pl.pallas_call(
        functools.partial(ffn_kernel, spots, (len(arrays), chans), aligned),
        grid=(hidden // block,),
        in_specs=[pl.BlockSpec(memory_space=pltpu.SMEM), whole(tokens.shape)]
        + [whole(value.shape) for value in arrays]
        + [whole(w.shape) for w in w_outs]
        + [pl.BlockSpec((width, block), lambda i: (0, i))] * 2
        + [pl.BlockSpec(memory_space=pltpu.HBM)],
        out_specs=[
            whole((rows, share if aligned else width)),
            pl.BlockSpec((rows, block), lambda i: (0, i)),
            whole((rows, share)),
        ],
        out_shape=[
            jax.ShapeDtypeStruct((rows, share if aligned else width), jnp.float32),
            jax.ShapeDtypeStruct((rows, hidden), jnp.bfloat16),
            jax.ShapeDtypeStruct((rows, share), jnp.bfloat16),
        ],
        scratch_shapes=[
            pltpu.VMEM((chans, rows, heads_width), jnp.bfloat16),
            pltpu.VMEM((rows, width), jnp.bfloat16),
            pltpu.VMEM((rows, hidden), jnp.bfloat16),
            pltpu.VMEM((hidden, share), jnp.bfloat16),
            pltpu.SemaphoreType.DMA,
        ],
        compiler_params=params(40, dimension_semantics=("arbitrary",)),
        cost_estimate=cost(4 * rows * width * hidden, 4 * width * hidden, rows * hidden),
        name="out_and_ffn",
    )(scalars, tokens, *arrays, *w_outs, ff_value, ff_gate, ff_down)


def down_kernel(target_ref, gated_ref, down_ref, out_ref, total):
    at = pl.program_id(0)
    part = dot_nn(gated_ref[...], down_ref[...])

    @pl.when(at == 0)
    def _():
        total[...] = part

    @pl.when(at > 0)
    def _():
        total[...] += part

    @pl.when(at == pl.num_programs(0) - 1)
    def _():
        out_ref[...] = total[...].astype(out_ref.dtype)


def down_project(target, gated, ff_down, share, dtype):
    rows, hidden = gated.shape
    if share % LANES != 0:
        ff_down = lax.dynamic_slice_in_dim(ff_down, target * share, share, 1)
        target = jnp.zeros_like(target)
    block = next(size for size in (1280, 640, 512, 256, 128, hidden) if hidden % size == 0)
    return pl.pallas_call(
        down_kernel,
        grid_spec=pltpu.PrefetchScalarGridSpec(
            num_scalar_prefetch=1,
            grid=(hidden // block,),
            in_specs=[
                pl.BlockSpec((rows, block), lambda k, target: (0, k)),
                pl.BlockSpec((block, share), lambda k, target: (k, target[0])),
            ],
            out_specs=pl.BlockSpec((rows, share), lambda k, target: (0, 0)),
            scratch_shapes=[pltpu.VMEM((rows, share), jnp.float32)],
        ),
        out_shape=jax.ShapeDtypeStruct((rows, share), dtype),
        compiler_params=params(20, dimension_semantics=("arbitrary",)),
        cost_estimate=cost(2 * rows * hidden * share, 2 * hidden * share),
        name="down_project",
    )(target.reshape(1), gated, ff_down)


def image_block(
    tokens, stale_k, stale_v, w_query, w_key, w_value, w_outs, ff_value, ff_gate, ff_down
):
    rows, width = tokens.shape
    head_count = w_query.shape[1] // HD
    patches = lax.axis_size("patch")
    chans = lax.axis_size("chan")
    group = 1
    while head_count % (2 * group) == 0 and patches % (2 * group) == 0:
        group *= 2
    assert group == head_count and group >= 2
    near = group // 2
    peers = patches // group
    patch_id = lax.axis_index("patch")
    chan_id = lax.axis_index("chan").astype(jnp.int32)
    member = (patch_id // peers).astype(jnp.int32).reshape(1)

    def partner(p, step):
        return ((p // peers) ^ step) * peers + p % peers

    def trade(value, step):
        if step == 0:
            return value
        return lax.ppermute(value, "patch", [(p, partner(p, step)) for p in range(patches)])

    def beside(value, step):
        pairs = [
            (p, p // peers * peers + (p % peers + step) % peers) for p in range(patches)
        ]
        return lax.ppermute(value, "patch", pairs)

    def over_chan(value, step):
        return lax.ppermute(value, "chan", [(c, (c + step) % chans) for c in range(chans)])

    def trade_over_chan(value, step, chan_step):
        if chan_step == 0:
            return trade(value, step)
        pairs = [
            (p * chans + c, partner(p, step) * chans + (c + chan_step) % chans)
            for p in range(patches)
            for c in range(chans)
        ]
        return lax.ppermute(value, ("patch", "chan"), pairs)

    made = project_qkv(
        member, tokens, stale_k, stale_v, w_query, w_key, w_value, near, group
    )
    nears = [trade(made[step], step) for step in range(near)]
    stale_far = pack_stale(member, stale_k, stale_v, tuple(range(near, group)))
    kv_far = [trade(stale_far[step - near], step) for step in range(near, group)]
    q_far = [trade(made[step], step) for step in range(near, group)]
    local = attend_local(made[near:group], made[group:])
    locals_ = [local if step == 0 else over_chan(local, step) for step in range(chans)]
    result_size = result_rows(rows // 2)
    near_side = [[beside(value, step) for value in nears] for step in range(1, peers)]
    far_side = [[beside(value, step) for value in kv_far] for step in range(1, peers)]
    stale_at = rows // 2 + rows
    near_own = [(value, stale_at) for value in nears]
    near_rest = [(value, stale_at) for side in near_side for value in side]
    far_own = [(value, 0) for value in kv_far]
    far_rest = [(value, 0) for side in far_side for value in side]

    packets = [[] for _ in range(chans)]
    state = attend(nears, near_own + near_rest, rows, 0, True, partial=True)
    heads = attend(nears, far_own + far_rest, rows, None, False, state=state)
    if group > 2:
        mine = [trade(value, at) for at, value in enumerate(heads)]
        joined = jnp.concatenate(mine, axis=0)
        for step in range(chans):
            value = joined if step == 0 else over_chan(joined, step)
            packets[step] += [(value, at * (rows // 2), None, 0) for at in range(near)]
    else:
        for step in range(chans):
            for at, value in enumerate(heads):
                sent = trade_over_chan(value, at, step)
                packets[step].append((sent, 0, None, 0))
    parts = 2 if group >= 8 else 1
    size = (group - near) // parts
    everything = far_own + near_own + far_rest + near_rest
    for part in range(parts):
        start = part * size
        asked = q_far[start : start + size]
        asked, heads = lax.optimization_barrier((asked, heads))
        heads = attend(asked, everything, rows, start, False, stats=True)
        steps = range(near + start, near + start + size)
        if part < parts - 1:
            mine = [trade(value, at) for at, value in zip(steps, heads)]
            joined = jnp.concatenate(mine, axis=0)
            for step in range(chans):
                value = joined if step == 0 else over_chan(joined, step)
                packets[step] += [
                    (value, at * result_size, locals_[step], (start + at) * result_size)
                    for at in range(size)
                ]
        else:
            for step in range(chans):
                for at, value in zip(steps, heads):
                    sent = trade_over_chan(value, at, step)
                    packets[step].append((sent, 0, locals_[step], (at - near) * result_size))

    share = width // chans
    target = (chan_id + 1) % chans
    scalars = jnp.stack([member[0], target, chan_id])
    resid, gated, part = out_and_ffn(
        scalars, tokens, packets, w_outs, ff_value, ff_gate, ff_down, share
    )
    arrived = [over_chan(part, 1)] if chans > 1 else []
    for step in range(2, chans):
        part = down_project((chan_id + step) % chans, gated, ff_down, share, jnp.bfloat16)
        arrived.append(over_chan(part, step))
    total = down_project(chan_id, gated, ff_down, share, jnp.float32)
    if resid.shape[1] != share:
        resid = lax.dynamic_slice_in_dim(resid, chan_id * share, share, 1)
    total = total + resid
    for part in arrived:
        total = total + part.astype(jnp.float32)
    return total.astype(jnp.bfloat16)


def per_device(
    tokens, stale_k, stale_v, w_query, w_key, w_value, w_out, ff_value, ff_gate, ff_down
):
    chans = lax.axis_size("chan")
    w_outs = [w_out]
    for step in range(1, chans):
        pairs = [(c, (c + step) % chans) for c in range(chans)]
        w_outs.append(lax.ppermute(w_out, "chan", pairs))
    images = [
        image_block(
            tokens[at],
            stale_k[at],
            stale_v[at],
            w_query,
            w_key,
            w_value,
            w_outs,
            ff_value,
            ff_gate,
            ff_down,
        )
        for at in range(tokens.shape[0])
    ]
    return jnp.stack(images)


def solution(mesh):
    return jax.shard_map(
        per_device,
        mesh=mesh,
        in_specs=(
            P(None, "patch", None),
            P(None, "patch", "chan"),
            P(None, "patch", "chan"),
            P(None, "chan"),
            P(None, "chan"),
            P(None, "chan"),
            P("chan", None),
            P(None, "chan"),
            P(None, "chan"),
            P("chan", None),
        ),
        out_specs=P(None, "patch", "chan"),
        check_vma=False,
    )
```

```python
import functools

import jax
import jax.numpy as jnp
from jax import lax
from jax.experimental import pallas as pl
from jax.experimental.pallas import tpu as pltpu
from jax.sharding import PartitionSpec as P


HD = 64
LANES = 128


def dot_nt(a, b):
    return lax.dot_general(a, b, (((1,), (1,)), ((), ())), preferred_element_type=jnp.float32)


def dot_nn(a, b):
    return jnp.dot(a, b, preferred_element_type=jnp.float32)


def swap(x):
    return jnp.concatenate([x[:, HD:], x[:, :HD]], axis=1)


def low_half(shape):
    return lax.broadcasted_iota(jnp.int32, shape, 1) < HD


def layer_norm(values):
    mean = jnp.mean(values, axis=-1, keepdims=True)
    centered = values - mean
    var = jnp.mean(centered * centered, axis=-1, keepdims=True)
    return centered * lax.rsqrt(var + 1e-05)


def whole(shape):
    return pl.BlockSpec(shape, lambda *_: (0,) * len(shape))


def params(mib, **more):
    return pltpu.CompilerParams(vmem_limit_bytes=mib * 2**20, **more)


def cost(flops, moved, trans=0):
    return pl.CostEstimate(flops=int(flops), bytes_accessed=int(moved), transcendentals=int(trans))


STAT_ROWS = 16


def write_result(out_ref, start, parts, with_stats):
    rows = parts[0][0].shape[0]
    low = low_half((rows, LANES))
    sides = [accum / swap(accum) for accum, _ in parts]
    out_ref[start : start + rows, :] = jnp.where(low, swap(sides[0]), sides[1]).astype(
        jnp.bfloat16
    )
    if not with_stats:
        return
    lane = lax.broadcasted_iota(jnp.int32, (rows, LANES), 1)
    table = jnp.zeros((rows, LANES), jnp.float32)
    for side, (accum, top) in enumerate(parts):
        rest = jnp.where(low, top + jnp.log(jnp.where(low, accum, 1.0)), 0.0)
        for part in range(3):
            piece = rest.astype(jnp.bfloat16).astype(jnp.float32)
            rest = rest - piece
            table = jnp.where(lane == 3 * side + part, piece, table)
    pick_shape = (STAT_ROWS, LANES)
    pick = lax.broadcasted_iota(jnp.int32, pick_shape, 0) == lax.broadcasted_iota(
        jnp.int32, pick_shape, 1
    )
    stats = dot_nt(
        jnp.where(pick, 1.0, 0.0).astype(jnp.bfloat16), table.astype(jnp.bfloat16)
    ).astype(jnp.bfloat16)
    for at in range(rows // LANES):
        first = start + rows + at * STAT_ROWS
        out_ref[first : first + STAT_ROWS, :] = stats[:, at * LANES : (at + 1) * LANES]


def result_rows(rows):
    return rows + rows // LANES * STAT_ROWS


def read_stats(ref, start, rows):
    stats = jnp.concatenate(
        [
            ref[start + rows + at * STAT_ROWS : start + rows + (at + 1) * STAT_ROWS, :]
            for at in range(rows // LANES)
        ],
        axis=1,
    )
    row = lax.broadcasted_iota(jnp.int32, (STAT_ROWS, LANES), 0)
    low = low_half((STAT_ROWS, LANES))
    spread = jnp.where((row < 3) & low | (row >= 3) & (row < 6) & ~low, 1.0, 0.0)
    return lax.dot_general(
        stats,
        spread.astype(jnp.bfloat16),
        (((0,), (0,)), ((), ())),
        preferred_element_type=jnp.float32,
    )


def merge_results(ref, start, local_ref, local_start, rows):
    one = ref[start : start + rows, :].astype(jnp.float32)
    two = local_ref[local_start : local_start + rows, :].astype(jnp.float32)
    gap = read_stats(local_ref, local_start, rows) - read_stats(ref, start, rows)
    share = 1.0 / (1.0 + jnp.exp(gap))
    return (two + (one - two) * share).astype(jnp.bfloat16)


def local_kernel(count, *refs):
    q_refs, fresh_refs = refs[:count], refs[count : 2 * count]
    out_ref, packed_ref, fresh_ref = refs[2 * count :]
    for at in range(count):

        @pl.when(pl.program_id(0) == at)
        def _(at=at):
            packed_ref[...] = q_refs[at][...]
            fresh_ref[...] = fresh_refs[at][...]

    packed, fresh = packed_ref[...], fresh_ref[...]
    low = low_half(packed.shape)
    fresh_v = jnp.where(low_half(fresh.shape), jnp.ones_like(fresh), fresh)
    zero = jnp.zeros_like(packed)
    parts = []
    for query in (jnp.where(low, packed, zero), jnp.where(low, swap(packed), zero)):
        scores = dot_nt(query, fresh)
        top = jnp.max(scores, axis=1, keepdims=True)
        parts.append((dot_nn(jnp.exp(scores - top).astype(jnp.bfloat16), fresh_v), top))
    write_result(out_ref, 0, parts, True)


def attend_local(queries, fresh):
    count, rows = len(queries), queries[0].shape[0]
    size = result_rows(rows)
    return pl.pallas_call(
        functools.partial(local_kernel, count),
        grid=(count,),
        in_specs=[whole(value.shape) for value in (*queries, *fresh)],
        out_specs=pl.BlockSpec((size, LANES), lambda i: (i, 0)),
        out_shape=jax.ShapeDtypeStruct((count * size, LANES), jnp.bfloat16),
        scratch_shapes=[
            pltpu.VMEM(queries[0].shape, jnp.bfloat16),
            pltpu.VMEM(fresh[0].shape, jnp.bfloat16),
        ],
        compiler_params=params(16, dimension_semantics=("arbitrary",)),
        cost_estimate=cost(16 * count * rows * rows * LANES, 8 * count * rows * LANES),
        name="attend_local",
    )(*queries, *fresh)


def head_tile(ref, head):
    return ref[:, pl.ds(pl.multiple_of((head // 2) * LANES, LANES), LANES)]


def pack_kv(member, step, k_ref, v_ref, store):
    head = jnp.bitwise_xor(member, step)

    def put(odd):
        k_tile, v_tile = head_tile(k_ref, head), head_tile(v_ref, head)
        low = low_half(k_tile.shape)
        store(jnp.where(low, swap(k_tile), v_tile) if odd else jnp.where(low, k_tile, swap(v_tile)))

    pl.when(head % 2 == 0)(lambda: put(False))
    pl.when(head % 2 == 1)(lambda: put(True))


def pack_kernel(steps, member_ref, k_ref, v_ref, *out_refs):
    for step, out in zip(steps, out_refs):

        def store(value, out=out):
            out[...] = value

        pack_kv(member_ref[0], step, k_ref, v_ref, store)


def pack_stale(member, stale_k, stale_v, steps):
    rows, width = stale_k.shape
    packet = jax.ShapeDtypeStruct((rows, LANES), jnp.bfloat16)
    return pl.pallas_call(
        functools.partial(pack_kernel, steps),
        in_specs=[
            pl.BlockSpec(memory_space=pltpu.SMEM),
            pl.BlockSpec(memory_space=pltpu.VMEM),
            pl.BlockSpec(memory_space=pltpu.VMEM),
        ],
        out_specs=[pl.BlockSpec(memory_space=pltpu.VMEM)] * len(steps),
        out_shape=[packet] * len(steps),
        compiler_params=params(8),
        cost_estimate=cost(1e9, 4 * rows * width * 2),
        name="pack_stale",
    )(member, stale_k, stale_v)


def qkv_kernel(near, group, member_ref, x_ref, k_ref, v_ref, wq_hbm, wk_hbm, wv_hbm, *rest):
    out_refs, rest = rest[:group], rest[group:]
    fresh_refs, (wq, wk, wv, qs, ks, vs, sems) = rest[: group - near], rest[group - near :]
    copies = [
        pltpu.make_async_copy(src, dst, sems.at[at])
        for at, (src, dst) in enumerate(((wq_hbm, wq), (wk_hbm, wk), (wv_hbm, wv)))
    ]
    for copy in copies:
        copy.start()
    rows = x_ref.shape[0]
    half = rows // 2
    member = member_ref[0]
    for step in range(near):

        def store_stale(value, out=out_refs[step]):
            out[half + rows :, :] = value

        pack_kv(member, step, k_ref, v_ref, store_stale)
    normed = layer_norm(x_ref[...].astype(jnp.float32)).astype(jnp.bfloat16)
    copies[0].wait()
    qs[...] = (dot_nn(normed, wq[...]).astype(jnp.bfloat16) * (1.0 / HD**0.5)).astype(jnp.bfloat16)
    copies[1].wait()
    ks[...] = dot_nn(normed, wk[...]).astype(jnp.bfloat16)
    copies[2].wait()
    vs[...] = dot_nn(normed, wv[...]).astype(jnp.bfloat16)
    for step in range(group):
        out = out_refs[step]
        head = jnp.bitwise_xor(member, step)

        def put(odd, out=out, head=head):
            tile = head_tile(qs, head)
            low = low_half((half, LANES))
            first, second = tile[:half], tile[half:]
            if odd:
                out[:half, :] = jnp.where(low, swap(first), second)
            else:
                out[:half, :] = jnp.where(low, first, swap(second))

        pl.when(head % 2 == 0)(functools.partial(put, False))
        pl.when(head % 2 == 1)(functools.partial(put, True))

        def store(value, out=out, step=step):
            if step < near:
                out[half : half + rows, :] = value
            else:
                fresh_refs[step - near][...] = value

        pack_kv(member, step, ks, vs, store)


def project_qkv(member, tokens, stale_k, stale_v, w_query, w_key, w_value, near, group):
    rows, width = tokens.shape
    out_width = w_query.shape[1]
    return pl.pallas_call(
        functools.partial(qkv_kernel, near, group),
        in_specs=[pl.BlockSpec(memory_space=pltpu.SMEM)]
        + [pl.BlockSpec(memory_space=pltpu.VMEM)] * 3
        + [pl.BlockSpec(memory_space=pltpu.HBM)] * 3,
        out_specs=[pl.BlockSpec(memory_space=pltpu.VMEM)] * (2 * group - near),
        out_shape=[
            jax.ShapeDtypeStruct((size, LANES), jnp.bfloat16)
            for size in [rows // 2 + 2 * rows] * near
            + [rows // 2] * (group - near)
            + [rows] * (group - near)
        ],
        scratch_shapes=[pltpu.VMEM((width, out_width), jnp.bfloat16)] * 3
        + [pltpu.VMEM((rows, out_width), jnp.bfloat16)] * 3
        + [pltpu.SemaphoreType.DMA((3,))],
        compiler_params=params(60),
        cost_estimate=cost(6 * rows * width * out_width, 2 * 3 * width * out_width),
        name="project_qkv",
    )(member, tokens, stale_k, stale_v, w_query, w_key, w_value)


def attend_kernel(plan, *refs):
    count, blocks, queries, kv_rows = plan["count"], plan["blocks"], plan["queries"], plan["rows"]
    arrays, refs = refs[: plan["arrays"]], refs[plan["arrays"] :]
    state_in, refs = (refs[:1], refs[1:]) if plan["resume"] else (None, refs)
    outs = 1 if plan["partial"] else count
    out_refs, (kvs, ones_v, qfs, result) = refs[:outs], refs[outs:]
    at = pl.program_id(0)
    half = kv_rows // 2
    low_kv = low_half((kv_rows, LANES))
    low_q = low_half((half, LANES))
    q_rows = qfs.shape[1]

    @pl.when(at == 0)
    def _():
        for b, (ref, start) in enumerate(blocks):
            block = arrays[ref][start : start + kv_rows, :]
            kvs[b] = block
            ones_v[b] = jnp.where(low_kv, jnp.ones_like(block), block)
        for i, ref in enumerate(queries):
            qfs[i] = arrays[ref][:q_rows, :]

    packed = qfs[at, :half, :]
    zero = jnp.zeros_like(packed)
    if plan["own"] is None:
        keys = [(kvs, ones_v, b) for b in range(len(blocks))]
    else:
        own = plan["own"] + at
        keys = [
            (kvs, ones_v, b + (b >= own).astype(jnp.int32)) for b in range(len(blocks) - 1)
        ]
    fresh, fresh_v = None, None
    if plan["fresh"]:
        fresh = qfs[at, half:, :]
        fresh_v = jnp.where(low_kv, jnp.ones_like(fresh), fresh)
    results = []
    for side, query in enumerate(
        (jnp.where(low_q, packed, zero), jnp.where(low_q, swap(packed), zero))
    ):
        scores = [dot_nt(query, ref[pick]) for ref, _, pick in keys]
        if fresh is not None:
            scores.append(dot_nt(query, fresh))
        top = scores[0]
        for block in scores[1:]:
            top = jnp.maximum(top, block)
        top = jnp.max(top, axis=1, keepdims=True)
        accum = None
        for b, block in enumerate(scores):
            weights = jnp.exp(block - top).astype(jnp.bfloat16)
            part = dot_nn(weights, keys[b][1][keys[b][2]] if b < len(keys) else fresh_v)
            accum = part if accum is None else accum + part
        if plan["resume"]:
            carried = state_in[0][0, side]
            top_in = carried[:, :1]
            accum_in = jnp.where(low_q, carried[:, HD - 1 : HD], carried)
            both = jnp.maximum(top_in, top)
            accum = accum_in * jnp.exp(top_in - both) + accum * jnp.exp(top - both)
        if plan["partial"]:
            lane = lax.broadcasted_iota(jnp.int32, (half, LANES), 1)
            out_refs[0][0, side] = jnp.where(lane < HD // 2, top, accum)
        else:
            results.append((accum, top))
    if not plan["partial"]:
        write_result(result, 0, results, plan["stats"])
        for i in range(count):

            @pl.when(at == i)
            def _(i=i):
                out_refs[i][...] = result[: out_refs[i].shape[0], :]


def attend(queries, kv_blocks, kv_rows, own, fresh, state=None, partial=False, stats=False):
    arrays = []

    def place(value):
        for at, known in enumerate(arrays):
            if known is value:
                return at
        arrays.append(value)
        return len(arrays) - 1

    count = len(queries)
    half = kv_rows // 2
    plan = {
        "count": count,
        "queries": [place(query) for query in queries],
        "blocks": [(place(value), start) for value, start in kv_blocks],
        "rows": kv_rows,
        "own": own,
        "resume": state is not None,
        "partial": partial,
        "fresh": fresh,
        "stats": stats,
    }
    plan["arrays"] = len(arrays)
    blocks = len(kv_blocks)
    pairs = count * 2 * half * blocks * kv_rows
    carried = pl.BlockSpec((1, 2, half, LANES), lambda i: (i, 0, 0, 0))
    if partial:
        out_specs = [carried]
        out_shape = [jax.ShapeDtypeStruct((count, 2, half, LANES), jnp.float32)]
    else:
        packet = (result_rows(half) if stats else half, LANES)
        out_specs = [whole(packet)] * count
        out_shape = [jax.ShapeDtypeStruct(packet, jnp.bfloat16)] * count
    return pl.pallas_call(
        functools.partial(attend_kernel, plan),
        grid=(count,),
        in_specs=[whole(value.shape) for value in arrays] + ([carried] if state else []),
        out_specs=out_specs,
        out_shape=out_shape,
        scratch_shapes=[
            pltpu.VMEM((blocks, kv_rows, LANES), jnp.bfloat16),
            pltpu.VMEM((blocks, kv_rows, LANES), jnp.bfloat16),
            pltpu.VMEM((count, half + kv_rows if fresh else half, LANES), jnp.bfloat16),
            pltpu.VMEM((result_rows(half), LANES), jnp.bfloat16),
        ],
        compiler_params=params(4 + blocks * kv_rows // 218, dimension_semantics=("arbitrary",)),
        cost_estimate=cost(4 * pairs * LANES, 2 * blocks * kv_rows * LANES, pairs),
    )(*arrays, *(state or ()))


def ffn_kernel(spots, counts, aligned, scalars_ref, tokens_ref, *refs):
    arrays, chans = counts
    packets, refs = refs[:arrays], refs[arrays:]
    w_out_refs, refs = refs[:chans], refs[chans:]
    val_ref, gate_ref, down_hbm, resid_ref, gated_ref, part_ref, *refs = refs
    heads, normed_two, gated_all, down, sem = refs
    rows = tokens_ref.shape[0]
    half = rows // 2
    at, last = pl.program_id(0), pl.num_programs(0) - 1
    share = part_ref.shape[1]
    member, target, chan = scalars_ref[0], scalars_ref[1], scalars_ref[2]

    def columns(index, size):
        return pl.ds(pl.multiple_of(index * size, LANES), size)

    down_src = down_hbm.at[:, columns(target, share)] if aligned else down_hbm
    down_copy = pltpu.make_async_copy(down_src, down, sem)

    @pl.when(at == 0)
    def _():
        down_copy.start()
        low = low_half((half, LANES))
        for c in range(chans):
            for pair in range(len(spots[c]) // 2):
                place = columns(jnp.bitwise_xor(member // 2, pair), LANES)

                def put(odd, pair=pair, place=place, c=c):
                    one, two = (
                        packets[ref][start : start + half, :]
                        if local is None
                        else merge_results(packets[ref], start, packets[local], local_start, half)
                        for ref, start, local, local_start in spots[c][2 * pair : 2 * pair + 2]
                    )
                    even_head, odd_head = (two, one) if odd else (one, two)
                    heads[c, :half, place] = jnp.where(low, even_head, swap(odd_head))
                    heads[c, half:, place] = jnp.where(low, swap(even_head), odd_head)

                pl.when(member % 2 == 0)(functools.partial(put, False))
                pl.when(member % 2 == 1)(functools.partial(put, True))
        resid = tokens_ref[...].astype(jnp.float32)
        for c in range(chans):
            resid = resid + dot_nn(heads[c], w_out_refs[c][...])
        if aligned:
            for c in range(chans):

                @pl.when(chan == c)
                def _(c=c):
                    resid_ref[...] = resid[:, c * share : (c + 1) * share]
        else:
            resid_ref[...] = resid
        normed_two[...] = layer_norm(resid).astype(jnp.bfloat16)

    block = gated_ref.shape[1]
    piece = block
    for start in range(0, block, piece):
        ff_val = dot_nn(normed_two[...], val_ref[:, start : start + piece])
        gate = dot_nn(normed_two[...], gate_ref[:, start : start + piece])
        gelu = 0.5 * gate * (1.0 + lax.erf(gate * (0.5**0.5)))
        gated = (ff_val * gelu).astype(jnp.bfloat16)
        gated_ref[:, start : start + piece] = gated
        gated_all[:, pl.ds(pl.multiple_of(at * block + start, LANES), piece)] = gated

    @pl.when(at == last)
    def _():
        down_copy.wait()
        part_ref[...] = dot_nn(gated_all[...], down[...]).astype(part_ref.dtype)


def out_and_ffn(scalars, tokens, packets, w_outs, ff_value, ff_gate, ff_down, share):
    rows, width = tokens.shape
    hidden = ff_value.shape[1]
    block = next(size for size in (512, 256, 128) if hidden % size == 0)
    chans = len(w_outs)
    heads_width = w_outs[0].shape[0]
    arrays, spots = [], []

    def place(value):
        if value is None:
            return None
        for at, known in enumerate(arrays):
            if known is value:
                return at
        arrays.append(value)
        return len(arrays) - 1

    for chan in packets:
        spots.append([])
        for value, start, local, local_start in chan:
            spots[-1].append((place(value), start, place(local), local_start))
    aligned = share % LANES == 0
    if not aligned:
        ff_down = lax.dynamic_slice_in_dim(ff_down, scalars[1] * share, share, 1)
    return pl.pallas_call(
        functools.partial(ffn_kernel, spots, (len(arrays), chans), aligned),
        grid=(hidden // block,),
        in_specs=[pl.BlockSpec(memory_space=pltpu.SMEM), whole(tokens.shape)]
        + [whole(value.shape) for value in arrays]
        + [whole(w.shape) for w in w_outs]
        + [pl.BlockSpec((width, block), lambda i: (0, i))] * 2
        + [pl.BlockSpec(memory_space=pltpu.HBM)],
        out_specs=[
            whole((rows, share if aligned else width)),
            pl.BlockSpec((rows, block), lambda i: (0, i)),
            whole((rows, share)),
        ],
        out_shape=[
            jax.ShapeDtypeStruct((rows, share if aligned else width), jnp.float32),
            jax.ShapeDtypeStruct((rows, hidden), jnp.bfloat16),
            jax.ShapeDtypeStruct((rows, share), jnp.bfloat16),
        ],
        scratch_shapes=[
            pltpu.VMEM((chans, rows, heads_width), jnp.bfloat16),
            pltpu.VMEM((rows, width), jnp.bfloat16),
            pltpu.VMEM((rows, hidden), jnp.bfloat16),
            pltpu.VMEM((hidden, share), jnp.bfloat16),
            pltpu.SemaphoreType.DMA,
        ],
        compiler_params=params(40, dimension_semantics=("arbitrary",)),
        cost_estimate=cost(4 * rows * width * hidden, 4 * width * hidden, rows * hidden),
        name="out_and_ffn",
    )(scalars, tokens, *arrays, *w_outs, ff_value, ff_gate, ff_down)


def down_kernel(target_ref, gated_ref, down_ref, out_ref, total):
    at = pl.program_id(0)
    part = dot_nn(gated_ref[...], down_ref[...])

    @pl.when(at == 0)
    def _():
        total[...] = part

    @pl.when(at > 0)
    def _():
        total[...] += part

    @pl.when(at == pl.num_programs(0) - 1)
    def _():
        out_ref[...] = total[...].astype(out_ref.dtype)


def down_project(target, gated, ff_down, share, dtype):
    rows, hidden = gated.shape
    if share % LANES != 0:
        ff_down = lax.dynamic_slice_in_dim(ff_down, target * share, share, 1)
        target = jnp.zeros_like(target)
    block = next(size for size in (1280, 640, 512, 256, 128, hidden) if hidden % size == 0)
    return pl.pallas_call(
        down_kernel,
        grid_spec=pltpu.PrefetchScalarGridSpec(
            num_scalar_prefetch=1,
            grid=(hidden // block,),
            in_specs=[
                pl.BlockSpec((rows, block), lambda k, target: (0, k)),
                pl.BlockSpec((block, share), lambda k, target: (k, target[0])),
            ],
            out_specs=pl.BlockSpec((rows, share), lambda k, target: (0, 0)),
            scratch_shapes=[pltpu.VMEM((rows, share), jnp.float32)],
        ),
        out_shape=jax.ShapeDtypeStruct((rows, share), dtype),
        compiler_params=params(20, dimension_semantics=("arbitrary",)),
        cost_estimate=cost(2 * rows * hidden * share, 2 * hidden * share),
        name="down_project",
    )(target.reshape(1), gated, ff_down)


def image_block(
    tokens, stale_k, stale_v, w_query, w_key, w_value, w_outs, ff_value, ff_gate, ff_down
):
    rows, width = tokens.shape
    head_count = w_query.shape[1] // HD
    patches = lax.axis_size("patch")
    chans = lax.axis_size("chan")
    group = 1
    while head_count % (2 * group) == 0 and patches % (2 * group) == 0:
        group *= 2
    assert group == head_count and group >= 2
    near = group // 2
    peers = patches // group
    patch_id = lax.axis_index("patch")
    chan_id = lax.axis_index("chan").astype(jnp.int32)
    member = (patch_id // peers).astype(jnp.int32).reshape(1)

    def partner(p, step):
        return ((p // peers) ^ step) * peers + p % peers

    def trade(value, step):
        if step == 0:
            return value
        return lax.ppermute(value, "patch", [(p, partner(p, step)) for p in range(patches)])

    def beside(value, step):
        pairs = [
            (p, p // peers * peers + (p % peers + step) % peers) for p in range(patches)
        ]
        return lax.ppermute(value, "patch", pairs)

    def over_chan(value, step):
        return lax.ppermute(value, "chan", [(c, (c + step) % chans) for c in range(chans)])

    def trade_over_chan(value, step, chan_step):
        if chan_step == 0:
            return trade(value, step)
        pairs = [
            (p * chans + c, partner(p, step) * chans + (c + chan_step) % chans)
            for p in range(patches)
            for c in range(chans)
        ]
        return lax.ppermute(value, ("patch", "chan"), pairs)

    made = project_qkv(
        member, tokens, stale_k, stale_v, w_query, w_key, w_value, near, group
    )
    nears = [trade(made[step], step) for step in range(near)]
    stale_far = pack_stale(member, stale_k, stale_v, tuple(range(near, group)))
    kv_far = [trade(stale_far[step - near], step) for step in range(near, group)]
    q_far = [trade(made[step], step) for step in range(near, group)]
    local = attend_local(made[near:group], made[group:])
    locals_ = [local if step == 0 else over_chan(local, step) for step in range(chans)]
    result_size = result_rows(rows // 2)
    near_side = [[beside(value, step) for value in nears] for step in range(1, peers)]
    far_side = [[beside(value, step) for value in kv_far] for step in range(1, peers)]
    stale_at = rows // 2 + rows
    near_own = [(value, stale_at) for value in nears]
    near_rest = [(value, stale_at) for side in near_side for value in side]
    far_own = [(value, 0) for value in kv_far]
    far_rest = [(value, 0) for side in far_side for value in side]

    packets = [[None] * group for _ in range(chans)]
    state = attend(nears, near_own + near_rest, rows, 0, True, partial=True)
    heads = attend(nears, far_own + far_rest, rows, None, False, state=state)
    if group > 2:
        mine = [trade(value, at) for at, value in enumerate(heads)]
        joined = jnp.concatenate(mine, axis=0)
        for step in range(chans):
            value = joined if step == 0 else over_chan(joined, step)
            packets[step][:near] = [(value, at * (rows // 2), None, 0) for at in range(near)]
    else:
        for step in range(chans):
            for at, value in enumerate(heads):
                sent = trade_over_chan(value, at, step)
                packets[step][at] = (sent, 0, None, 0)
    parts = 2 if group >= 8 else 1
    size = (group - near) // parts
    everything = far_own + near_own + far_rest + near_rest
    for part in range(parts):
        start = (parts - 1 - part) * size
        asked = q_far[start : start + size]
        asked, heads = lax.optimization_barrier((asked, heads))
        heads = attend(asked, everything, rows, start, False, stats=True)
        steps = range(near + start, near + start + size)
        if part < parts - 1:
            mine = [trade(value, at) for at, value in zip(steps, heads)]
            joined = jnp.concatenate(mine, axis=0)
            for step in range(chans):
                value = joined if step == 0 else over_chan(joined, step)
                packets[step][near + start : near + start + size] = [
                    (value, at * result_size, locals_[step], (start + at) * result_size)
                    for at in range(size)
                ]
        else:
            for step in range(chans):
                for at, value in zip(steps, heads):
                    sent = trade_over_chan(value, at, step)
                    packets[step][at] = (sent, 0, locals_[step], (at - near) * result_size)

    share = width // chans
    target = (chan_id + 1) % chans
    scalars = jnp.stack([member[0], target, chan_id])
    resid, gated, part = out_and_ffn(
        scalars, tokens, packets, w_outs, ff_value, ff_gate, ff_down, share
    )
    arrived = [over_chan(part, 1)] if chans > 1 else []
    for step in range(2, chans):
        part = down_project((chan_id + step) % chans, gated, ff_down, share, jnp.bfloat16)
        arrived.append(over_chan(part, step))
    total = down_project(chan_id, gated, ff_down, share, jnp.float32)
    if resid.shape[1] != share:
        resid = lax.dynamic_slice_in_dim(resid, chan_id * share, share, 1)
    total = total + resid
    for part in arrived:
        total = total + part.astype(jnp.float32)
    return total.astype(jnp.bfloat16)


def per_device(
    tokens, stale_k, stale_v, w_query, w_key, w_value, w_out, ff_value, ff_gate, ff_down
):
    chans = lax.axis_size("chan")
    w_outs = [w_out]
    for step in range(1, chans):
        pairs = [(c, (c + step) % chans) for c in range(chans)]
        w_outs.append(lax.ppermute(w_out, "chan", pairs))
    images = [
        image_block(
            tokens[at],
            stale_k[at],
            stale_v[at],
            w_query,
            w_key,
            w_value,
            w_outs,
            ff_value,
            ff_gate,
            ff_down,
        )
        for at in range(tokens.shape[0])
    ]
    return jnp.stack(images)


def solution(mesh):
    return jax.shard_map(
        per_device,
        mesh=mesh,
        in_specs=(
            P(None, "patch", None),
            P(None, "patch", "chan"),
            P(None, "patch", "chan"),
            P(None, "chan"),
            P(None, "chan"),
            P(None, "chan"),
            P("chan", None),
            P(None, "chan"),
            P(None, "chan"),
            P("chan", None),
        ),
        out_specs=P(None, "patch", "chan"),
        check_vma=False,
    )
```
